512 devices in a mesh: tm: 32 (over z, core), batch: 16 (over x, y).
Axes of the slice: x: 4, y: 4, z: 16, core: 2. Of those that a mesh axis runs over, the one named last changes fastest.
Arguments:
- rewards: float32 [2048, 32768], P('batch', 'tm'), may hold values from -0.12 to 0.12
- values: float32 [2048, 32768], P('batch', 'tm'), may hold values from -3 to 3
- episode_ends: int32 [2048, 32768], P('batch', 'tm'), may hold values 0 or 1
- lengths: int32 [2048], P('batch'), may hold values from 8192 to 32768
- groups: int32 [2048], P('batch'), may hold values from 0 to 127, as said below
Outputs:
- advantages: float32 [2048, 32768], P('batch', 'tm')
- grouped_advantages: float32 [2048, 32768], P('batch', 'tm')
- grouped_returns: float32 [2048, 32768], P('batch', 'tm')
The draws below stay inside these ranges and needn't reach their ends.
Inputs may be any that keep to these rules, and one draw needn't show every extreme that they name: `groups`: every group has exactly one rollout in each aligned block of 128 rollouts.
All inputs are finite; a program needn't handle non-finite values. No bound on the sum of `episode_ends` on one device may be relied on, other than what follows from the above.
Results may differ from the reference program's by a relative error of at most 0.0003.
Values sent between devices are 32-bit elements; how exact they have to be, the bound alone decides.
A program may use at most 64 MiB of HBM per device.

```python
import jax
import jax.numpy as jnp
from jax import lax

B_DEV = 128
GROUP = 16
ROLL = 2048
LENGTH = 32768
NGROUPS = 128
N_BATCH = 16


def draw_groups(key, part):
    members = GROUP // N_BATCH
    keys = jax.random.split(jax.random.fold_in(key, 7), N_BATCH + 1)

    def local_slots(subkey):
        return jax.random.permutation(subkey, B_DEV) // members
    slots = jax.vmap(local_slots)(keys[:N_BATCH])
    relabel = jax.random.permutation(keys[N_BATCH], NGROUPS)
    return relabel[slots.reshape(-1)].astype(jnp.int32)


def with_ends(values, own_key, low, largest):
    place = [jax.random.randint(jax.random.fold_in(own_key, axis), (), 0, length) for axis, length in enumerate(values.shape)]
    longest = values.shape.index(max(values.shape))
    next_to = place[:longest] + [(place[longest] + 1) % values.shape[longest]] + place[longest + 1:]
    return values.at[tuple(place)].set(low).at[tuple(next_to)].set(largest)


def steps_of(key, shape, shards, least, top_value):
    def one(axis_at, blocks):
        heights = jax.random.uniform(jax.random.fold_in(jax.random.fold_in(key, 6), axis_at), (blocks,), jnp.float32, least / len(shards), top_value / len(shards))
        return jnp.repeat(jnp.exp(heights), shape[axis_at] // blocks).reshape((-1,) + (1,) * (len(shape) - axis_at - 1))

    level = one(*shards[0])
    for cut in shards[1:]:
        level = level * one(*cut)
    return level


def gaussian(stream_key, extent, width, bound, cuts=(), held_as=jnp.bfloat16):
    level = steps_of(stream_key, extent, cuts, -0.22, 0.18) if cuts else 1.0
    values = jax.random.normal(stream_key, extent, jnp.float32) * width * level
    return jnp.minimum(jnp.maximum(values, -bound), bound).astype(held_as)


def setup_inputs(seed: int = 0) -> dict:
    key_of = jax.random.split(jax.random.key(seed), 6)
    return {
        "rewards": gaussian(key_of[0], (ROLL, LENGTH), 0.02, 0.12, ((0, 16), (1, 32)), jnp.float32),
        "values": gaussian(key_of[1], (ROLL, LENGTH), 0.5, 3.0, ((0, 16), (1, 32)), jnp.float32),
        "episode_ends": with_ends((jax.random.randint(key_of[2], (ROLL, LENGTH), 0, LENGTH) < 8).astype(jnp.int32), jax.random.fold_in(key_of[2], 1), 0, 1),
        "lengths": with_ends(jax.random.randint(key_of[3], (ROLL,), LENGTH // 4, LENGTH + 1), jax.random.fold_in(key_of[3], 1), LENGTH // 4, LENGTH).astype(jnp.int32),
        "groups": draw_groups(jax.random.fold_in(key_of[5], 71), 0),
    }


GAMMA_RATE = 0.9995
ALPHA_RATE = 0.05
EPSILON = 1e-06

def compose(earlier, later):
    return (later[0] * earlier[0], later[1] + later[0] * earlier[1], later[2] * earlier[2], later[3] + later[2] * earlier[3])

def chain_terms(rewards, values, episode_ends, lengths, next_first, start):
    positions = start + lax.broadcasted_iota(jnp.int32, rewards.shape, 1)
    limit = lengths[:, None]
    inside = positions < limit
    final = (episode_ends == 1) | (positions == limit - 1)
    carry_on = jnp.where(inside & jnp.logical_not(final), 1.0, 0.0).astype(rewards.dtype)
    value_next = jnp.concatenate([values[:, 1:], next_first], axis=1)
    reward_in = jnp.where(inside, rewards, 0.0)
    delta = jnp.where(inside, reward_in + GAMMA_RATE * carry_on * value_next - values, 0.0)
    lambdas = 1.0 - 1.0 / (ALPHA_RATE * lengths.astype(rewards.dtype))
    return (GAMMA_RATE * carry_on, reward_in, GAMMA_RATE * lambdas[:, None] * carry_on, delta)

def reverse_scan(terms):
    flipped = tuple((jnp.flip(item, 1) for item in terms))
    summed = lax.associative_scan(compose, flipped, axis=1)
    return tuple((jnp.flip(item, 1) for item in summed))

def reference(rewards, values, episode_ends, lengths, groups):

    def one_block(index):
        first = (index * GROUP).astype(jnp.int32)
        rew_block = lax.dynamic_slice_in_dim(rewards, first, GROUP, 0)
        val_block = lax.dynamic_slice_in_dim(values, first, GROUP, 0)
        end_block = lax.dynamic_slice_in_dim(episode_ends, first, GROUP, 0)
        len_block = lax.dynamic_slice_in_dim(lengths, first, GROUP, 0)
        next_first = jnp.zeros((GROUP, 1), rewards.dtype)
        terms = chain_terms(rew_block, val_block, end_block, len_block, next_first, 0)
        scanned = reverse_scan(terms)
        return (scanned[1], scanned[3])
    block_ids = jnp.arange(ROLL // GROUP, dtype=jnp.int32)
    returns, advantages = lax.map(one_block, block_ids)
    returns = returns.reshape(ROLL, LENGTH)
    advantages = advantages.reshape(ROLL, LENGTH)
    onehot = (groups[:, None] == jnp.arange(NGROUPS, dtype=jnp.int32)[None, :]).astype(rewards.dtype)
    counts = jnp.dot(lengths.astype(rewards.dtype), onehot, precision=lax.Precision.HIGHEST)
    sums = jnp.dot(lax.optimization_barrier(jnp.sum(advantages, 1)), onehot, precision=lax.Precision.HIGHEST)
    squares = jnp.dot(lax.optimization_barrier(jnp.sum(advantages * advantages, 1)), onehot, precision=lax.Precision.HIGHEST)
    group_mean = sums / counts
    group_var = squares / counts - group_mean * group_mean
    row_mean = jnp.dot(onehot, group_mean, precision=lax.Precision.HIGHEST)
    row_var = jnp.dot(onehot, group_var, precision=lax.Precision.HIGHEST)
    positions = lax.broadcasted_iota(jnp.int32, (ROLL, LENGTH), 1)
    inside = positions < lengths[:, None]
    normalized = jnp.where(inside, (advantages - row_mean[:, None]) / jnp.sqrt(row_var[:, None] + EPSILON), 0.0)
    order = jnp.argsort(groups, stable=True).astype(jnp.int32)
    return (advantages, normalized[order], returns[order])
```

```python
import jax
import jax.numpy as jnp
from jax import lax
from jax.experimental import pallas as pl
from jax.experimental.pallas import tpu as pltpu
from jax.sharding import PartitionSpec as P

MESH = pl.DeviceIdType.MESH
F32 = jnp.float32
BF16 = jnp.bfloat16
GAMMA_RATE = 0.9995
ALPHA_RATE = 0.05
EPSILON = 1e-06
LANES = 128
TILE = 8
GROUP_ROWS = 16


def second_rate(lengths):
    return GAMMA_RATE * (1.0 - 1.0 / (ALPHA_RATE * lengths))


def squarings(rate, count):
    powers = [rate]
    for _ in range(count):
        powers.append(powers[-1] * powers[-1])
    return powers


def lane_powers(powers, exponent):
    result = None
    for bit, power in enumerate(powers):
        factor = jnp.where((exponent & (1 << bit)) != 0, power, 1.0)
        result = factor if result is None else result * factor
    return result


def split(value, terms):
    pieces = []
    for _ in range(terms):
        piece = value.astype(BF16)
        pieces.append(piece)
        value = value - piece.astype(F32)
    return pieces


def fused(
    n_tm,
    n_batch,
    len_ref,
    grp_ref,
    rew_hbm,
    val_hbm,
    end_hbm,
    adv_out,
    gadv_out,
    gret_out,
    rew,
    val,
    end,
    loc_r,
    loc_a,
    tail_a,
    len_cols,
    summary,
    send_bulk,
    recv_bulk,
    send_z,
    recv_z,
    send_stat,
    recv_stat,
    done_r,
    done_a,
    in_sem,
    out_sem,
    bulk_ss,
    bulk_rs,
    z_ss,
    z_rs,
    stat_ss,
    stat_rs,
    ready_sem,
):
    height, span = rew.shape
    count = span // LANES
    chunks = 4
    chunk_rows = height // chunks
    tm = lax.axis_index("tm")
    me = lax.axis_index("batch")
    core = lax.rem(tm, 2)
    partner = tm + 1 - 2 * core
    start = tm * span

    def loads(k):
        rows = pl.ds(k * chunk_rows, chunk_rows)
        return [
            pltpu.make_async_copy(source.at[rows, :], target.at[rows, :], in_sem.at[k, n])
            for n, (source, target) in enumerate(((rew_hbm, rew), (val_hbm, val), (end_hbm, end)))
        ]

    for k in range(chunks):
        for copy in loads(k):
            copy.start()

    barrier = pltpu.get_barrier_semaphore()
    for d in range(1, n_batch):
        pl.semaphore_signal(
            barrier,
            inc=1,
            device_id={"tm": tm - core, "batch": lax.rem(me + d, n_batch)},
            device_id_type=MESH,
        )
    for d in range(1, n_tm // 2):
        pl.semaphore_signal(
            barrier,
            inc=1,
            device_id={"tm": lax.rem(tm - core + 2 * d, n_tm) + 1, "batch": me},
            device_id_type=MESH,
        )
    pl.semaphore_signal(
        barrier, inc=1, device_id={"tm": partner, "batch": me}, device_id_type=MESH
    )

    lane_row = lax.broadcasted_iota(jnp.int32, (1, LANES), 1)
    lengths_row = len_ref[...]
    len_cols[...] = jnp.broadcast_to(lengths_row, (height, LANES)).T

    lane = lax.broadcasted_iota(jnp.int32, (GROUP_ROWS, LANES), 1)
    lane_f = lane.astype(F32)
    gamma_powers = [GAMMA_RATE ** (1 << bit) for bit in range(8)]
    up_r = lane_powers(gamma_powers[:7], lane)
    down_r = 1.0 / up_r
    to_end_r = down_r * gamma_powers[7]

    def scan_rows(g, _):
        rows = pl.ds(pl.multiple_of(g * GROUP_ROWS, GROUP_ROWS), GROUP_ROWS)
        lengths = len_cols[rows, :]
        rate = second_rate(lengths.astype(F32))
        powers = squarings(rate, 7)
        up_a = lane_powers(powers[:7], lane)
        down_a = 1.0 / up_a
        to_end_a = down_a * powers[7]
        limit = lengths - start
        rolled_next = None
        state = []
        last_break = None
        for j in reversed(range(count)):
            cols = pl.ds(j * LANES, LANES)
            place = lane + j * LANES
            reward, value, ends = rew[rows, cols], val[rows, cols], end[rows, cols]
            inside = place < limit
            carry_on = (place < limit - 1) & (ends != 1)
            rolled = pltpu.roll(value, LANES - 1, 1)
            after = 0.0 if rolled_next is None else rolled_next
            value_next = jnp.where(lane == LANES - 1, after, rolled)
            rolled_next = rolled
            reward_in = jnp.where(inside, reward, 0.0)
            follow = jnp.where(carry_on, value_next, 0.0)
            delta = jnp.where(inside, reward_in + GAMMA_RATE * follow - value, 0.0)
            stop = jnp.where(carry_on, float(LANES), lane_f)
            here = jnp.where(carry_on, -1.0, lane_f + float(j * LANES))
            last_break = here if last_break is None else jnp.maximum(last_break, here)
            for bit in range(7):
                step = 1 << bit
                moved = pltpu.roll(stop, LANES - step, 1)
                stop = jnp.minimum(stop, jnp.where(lane < LANES - step, moved, float(LANES)))
            reach = jnp.minimum(stop, float(LANES - 1)) - lane_f
            open_end = stop == float(LANES)
            sum_r, sum_a = reward_in * up_r, delta * up_a
            for bit in range(7):
                step = 1 << bit
                linked = reach >= float(step)
                sum_r = sum_r + jnp.where(linked, pltpu.roll(sum_r, LANES - step, 1), 0.0)
                sum_a = sum_a + jnp.where(linked, pltpu.roll(sum_a, LANES - step, 1), 0.0)
            state.append((j, sum_r * down_r, sum_a * down_a, open_end))
        final_break = jnp.max(last_break, axis=1, keepdims=True)
        carry_r = carry_a = None
        scale = to_end_a
        totals = None
        for j, part_r, part_a, open_end in state:
            cols = pl.ds(j * LANES, LANES)
            if carry_r is not None:
                part_r = part_r + jnp.where(open_end, to_end_r, 0.0) * carry_r
                part_a = part_a + jnp.where(open_end, to_end_a, 0.0) * carry_a
                scale = scale * powers[7]
            carry_r = jnp.broadcast_to(part_r[:, :1], part_r.shape)
            carry_a = jnp.broadcast_to(part_a[:, :1], part_a.shape)
            tail = jnp.where(lane_f + float(j * LANES) > final_break, scale, 0.0)
            loc_r[rows, cols] = part_r
            loc_a[rows, cols] = part_a
            tail_a[rows, cols] = tail
            terms = (part_a, part_a * part_a, part_a * tail, tail, tail * tail)
            totals = terms if totals is None else [s + t for s, t in zip(totals, terms)]
        first_value = jnp.broadcast_to(val[rows, pl.ds(0, LANES)][:, :1], carry_a.shape)
        columns = [carry_r, carry_a + first_value * (GAMMA_RATE / rate), float(span - 1) - final_break]
        columns += [jnp.sum(total, axis=1, keepdims=True) for total in totals]
        line = jnp.zeros((GROUP_ROWS, LANES), F32)
        for n, column in enumerate(columns):
            line = jnp.where(lane == n, column, line)
        summary[rows, :] = line
        return 0

    per_chunk = chunk_rows // GROUP_ROWS
    for k in range(chunks):
        for copy in loads(k):
            copy.wait()
        lax.fori_loop(k * per_chunk, (k + 1) * per_chunk, scan_rows, 0)

    send_z[...] = summary[...].T[:TILE]
    recv_z[tm] = send_z[...]

    order = lax.broadcasted_iota(jnp.int32, (height, height), 0) == jnp.broadcast_to(
        grp_ref[...], (height, height)
    )
    order = jnp.where(order, 1.0, 0.0).astype(BF16)
    twice = jnp.concatenate([order, order], axis=1)
    thrice = jnp.concatenate([order, order, order], axis=1)
    wide = 2 * LANES

    def permute(c, _):
        cols = pl.ds(pl.multiple_of(c * wide, wide), wide)
        for n, source in enumerate((loc_r, loc_a)):
            pieces = jnp.concatenate(split(source[:, cols], 2), axis=0)
            moved = jnp.dot(twice, pieces, preferred_element_type=F32)
            send_bulk[:, n * TILE : (n + 1) * TILE, cols] = moved.reshape(n_batch, TILE, wide)
        return 0

    lax.fori_loop(0, span // wide, permute, 0)

    @pl.when(core == 0)
    def _():
        pl.semaphore_wait(barrier, 2 * n_batch - 1)
        pl.semaphore_signal(
            ready_sem, inc=1, device_id={"tm": partner, "batch": me}, device_id_type=MESH
        )

    @pl.when(core == 1)
    def _():
        pl.semaphore_wait(ready_sem, 1)

    def bulk(to, slot):
        return pltpu.make_async_remote_copy(
            src_ref=send_bulk.at[to],
            dst_ref=recv_bulk.at[slot],
            send_sem=bulk_ss.at[to],
            recv_sem=bulk_rs.at[slot],
            device_id={"tm": tm, "batch": to},
            device_id_type=MESH,
        )

    def send_one(d, _):
        bulk(lax.rem(me + d, n_batch), me).start()
        return 0

    lax.fori_loop(1, n_batch, send_one, 0)

    @pl.when(core == 1)
    def _():
        pl.semaphore_wait(barrier, n_tm - 1)
        pl.semaphore_signal(
            ready_sem, inc=1, device_id={"tm": partner, "batch": me}, device_id_type=MESH
        )

    @pl.when(core == 0)
    def _():
        pl.semaphore_wait(ready_sem, 1)

    def along(to, slot):
        return pltpu.make_async_remote_copy(
            src_ref=send_z,
            dst_ref=recv_z.at[slot],
            send_sem=z_ss.at[to],
            recv_sem=z_rs.at[slot],
            device_id={"tm": to, "batch": me},
            device_id_type=MESH,
        )

    def tell_one(d, _):
        along(lax.rem(tm + d, n_tm), tm).start()
        return 0

    lax.fori_loop(1, n_tm, tell_one, 0)
    recv_bulk[me] = send_bulk[me]

    def hear_one(d, _):
        along(lax.rem(tm + d, n_tm), lax.rem(tm + d, n_tm)).wait_recv()
        return 0

    lax.fori_loop(1, n_tm, hear_one, 0)

    lengths_f = lengths_row.astype(F32)
    whole_a = squarings(second_rate(lengths_f), 10)[10]
    whole_r = GAMMA_RATE**span
    whole_a = jnp.broadcast_to(whole_a, (TILE, LANES))
    zero = whole_a * 0.0

    def chain(k, carried):
        block = n_tm - 1 - k
        into_r, into_a, own_r, own_a, first, second = carried
        tile = recv_z[block]
        piece = [jnp.broadcast_to(tile[n : n + 1], (TILE, LANES)) for n in range(TILE)]
        mine = jnp.where(block == tm, 1.0, 0.0)
        own_r = own_r + mine * into_r
        own_a = own_a + mine * into_a
        first = first + piece[3] + piece[6] * into_a
        second = second + piece[4] + into_a * (2.0 * piece[5] + piece[7] * into_a)
        whole = piece[2] == float(span)
        into_r = piece[0] + jnp.where(whole, whole_r, 0.0) * into_r
        into_a = piece[1] + jnp.where(whole, whole_a, 0.0) * into_a
        return into_r, into_a, own_r, own_a, first, second

    _, _, own_r, own_a, first, second = lax.fori_loop(0, n_tm, chain, (zero,) * 6)
    lines = jnp.concatenate(
        [line[:1] for line in (own_r, own_a, first, second, send_z[2:3], lengths_f)]
        + [jnp.zeros((height - 6, LANES), F32)],
        axis=0,
    )
    send_stat[...] = lax.dot_general(
        thrice,
        jnp.concatenate(split(lines, 3), axis=1),
        (((1,), (1,)), ((), ())),
        preferred_element_type=F32,
    )
    recv_stat[me] = send_stat[pl.ds(pl.multiple_of(me * TILE, TILE), TILE), :]

    def stat(to, slot):
        return pltpu.make_async_remote_copy(
            src_ref=send_stat.at[pl.ds(pl.multiple_of(to * TILE, TILE), TILE), :],
            dst_ref=recv_stat.at[slot],
            send_sem=stat_ss.at[to],
            recv_sem=stat_rs.at[slot],
            device_id={"tm": tm, "batch": to},
            device_id_type=MESH,
        )

    def send_stats(d, _):
        stat(lax.rem(me + d, n_batch), me).start()
        return 0

    lax.fori_loop(1, n_batch, send_stats, 0)

    summary[...] = lines.T

    def own_rows(g, _):
        rows = pl.ds(pl.multiple_of(g * GROUP_ROWS, GROUP_ROWS), GROUP_ROWS)
        into = jnp.broadcast_to(summary[rows, :][:, 1:2], (GROUP_ROWS, LANES))
        for j in range(count):
            cols = pl.ds(j * LANES, LANES)
            end_values = loc_a[rows, cols] + tail_a[rows, cols] * into
            loc_a[rows, cols] = end_values
        return 0

    lax.fori_loop(0, height // GROUP_ROWS, own_rows, 0)
    own_copy = pltpu.make_async_copy(loc_a, adv_out, out_sem.at[0])
    own_copy.start()

    def hear_stats(d, _):
        slot = lax.rem(me + d, n_batch)
        stat(slot, slot).wait_recv()
        return 0

    lax.fori_loop(1, n_batch, hear_stats, 0)
    total = recv_stat[0]
    for i in range(1, n_batch):
        total = total + recv_stat[i]
    counted = total[:, 5:6]
    mean = total[:, 2:3] / counted
    var = total[:, 3:4] / counted - mean * mean
    mean = jnp.broadcast_to(mean, (TILE, LANES))
    inverse = jnp.broadcast_to(1.0 / jnp.sqrt(var + EPSILON), (TILE, LANES))

    def finish(d, _):
        i = lax.rem(me + d, n_batch)

        @pl.when(d > 0)
        def _():
            bulk(i, i).wait_recv()

        facts = recv_stat[i]
        into_r = jnp.broadcast_to(facts[:, 0:1], (TILE, LANES))
        into_a = jnp.broadcast_to(facts[:, 1:2], (TILE, LANES))
        last = float(span - 1) - jnp.broadcast_to(facts[:, 4:5], (TILE, LANES))
        lengths = jnp.broadcast_to(facts[:, 5:6], (TILE, LANES))
        powers = squarings(second_rate(lengths), 7)
        scale_a = powers[7] / lane_powers(powers[:7], lane[:TILE])
        scale_r = to_end_r[:TILE]
        limit = lengths - start.astype(F32)
        rows = pl.ds(i, TILE, stride=n_batch)
        for j in reversed(range(count)):
            cols = pl.ds(j * LANES, LANES)
            place = lane_f[:TILE] + float(j * LANES)
            carried = place > last
            ret = recv_bulk[i, :TILE, cols] + jnp.where(carried, scale_r, 0.0) * into_r
            adv = recv_bulk[i, TILE:, cols] + jnp.where(carried, scale_a, 0.0) * into_a
            done_r[j, rows, :] = ret
            done_a[j, rows, :] = jnp.where(place < limit, (adv - mean) * inverse, 0.0)
            scale_r = scale_r * gamma_powers[7]
            scale_a = scale_a * powers[7]
        return 0

    lax.fori_loop(0, n_batch, finish, 0)

    def stores(j):
        cols = pl.ds(j * LANES, LANES)
        return [
            pltpu.make_async_copy(source.at[j], target.at[:, cols], out_sem.at[1 + 2 * j + n])
            for n, (source, target) in enumerate(((done_r, gret_out), (done_a, gadv_out)))
        ]

    for j in range(count):
        for copy in stores(j):
            copy.start()

    def sent(d, _):
        to = lax.rem(me + d, n_batch)
        bulk(to, me).wait_send()
        stat(to, me).wait_send()
        return 0

    lax.fori_loop(1, n_batch, sent, 0)

    def told(d, _):
        along(lax.rem(tm + d, n_tm), tm).wait_send()
        return 0

    lax.fori_loop(1, n_tm, told, 0)
    own_copy.wait()
    for j in range(count):
        for copy in stores(j):
            copy.wait()


def solution(mesh):
    n_tm, n_batch = mesh.shape["tm"], mesh.shape["batch"]

    def on_device(rewards, values, episode_ends, lengths, groups):
        height, span = rewards.shape
        block = pltpu.VMEM((height, span), F32)
        square = pltpu.VMEM((height, LANES), F32)
        out = jax.ShapeDtypeStruct((height, span), F32)

        def kernel(*refs):
            fused(n_tm, n_batch, *refs)

        return pl.pallas_call(
            kernel,
            out_shape=(out, out, out),
            in_specs=[pl.BlockSpec(memory_space=pltpu.VMEM)] * 2
            + [pl.BlockSpec(memory_space=pl.ANY)] * 3,
            out_specs=[pl.BlockSpec(memory_space=pl.ANY)] * 3,
            scratch_shapes=[
                block,
                block,
                pltpu.VMEM((height, span), jnp.int32),
                block,
                block,
                block,
                pltpu.VMEM((height, LANES), jnp.int32),
                square,
                pltpu.VMEM((n_batch, 2 * TILE, span), F32),
                pltpu.VMEM((n_batch, 2 * TILE, span), F32),
                pltpu.VMEM((TILE, LANES), F32),
                pltpu.VMEM((n_tm, TILE, LANES), F32),
                square,
                pltpu.VMEM((n_batch, TILE, LANES), F32),
                pltpu.VMEM((span // LANES, height, LANES), F32),
                pltpu.VMEM((span // LANES, height, LANES), F32),
                pltpu.SemaphoreType.DMA((4, 3)),
                pltpu.SemaphoreType.DMA((1 + 2 * (span // LANES),)),
                pltpu.SemaphoreType.DMA((n_batch,)),
                pltpu.SemaphoreType.DMA((n_batch,)),
                pltpu.SemaphoreType.DMA((n_tm,)),
                pltpu.SemaphoreType.DMA((n_tm,)),
                pltpu.SemaphoreType.DMA((n_batch,)),
                pltpu.SemaphoreType.DMA((n_batch,)),
                pltpu.SemaphoreType.REGULAR,
            ],
            compiler_params=pltpu.CompilerParams(collective_id=0, has_side_effects=True),
        )(lengths.reshape(1, height), groups.reshape(1, height), rewards, values, episode_ends)

    return jax.shard_map(
        on_device,
        mesh=mesh,
        in_specs=(
            P("batch", "tm"),
            P("batch", "tm"),
            P("batch", "tm"),
            P("batch"),
            P("batch"),
        ),
        out_specs=(P("batch", "tm"), P("batch", "tm"), P("batch", "tm")),
        check_vma=False,
    )
```

```python
import jax
import jax.numpy as jnp
from jax import lax
from jax.experimental import pallas as pl
from jax.experimental.pallas import tpu as pltpu
from jax.sharding import PartitionSpec as P

MESH = pl.DeviceIdType.MESH
F32 = jnp.float32
BF16 = jnp.bfloat16
GAMMA_RATE = 0.9995
ALPHA_RATE = 0.05
EPSILON = 1e-06
LANES = 128
TILE = 8
STRIDE = 136


def second_rate(lengths):
    return GAMMA_RATE * (1.0 - 1.0 / (ALPHA_RATE * lengths))


def squarings(rate, count):
    powers = [rate]
    for _ in range(count):
        powers.append(powers[-1] * powers[-1])
    return powers


def lane_powers(powers, exponent):
    result = None
    for bit, power in enumerate(powers):
        factor = jnp.where((exponent & (1 << bit)) != 0, power, 1.0)
        result = factor if result is None else result * factor
    return result


def split(value, terms):
    pieces = []
    for _ in range(terms):
        piece = value.astype(BF16)
        pieces.append(piece)
        value = value - piece.astype(F32)
    return pieces


def fused(
    n_tm,
    n_batch,
    len_ref,
    grp_ref,
    rew_hbm,
    val_hbm,
    end_hbm,
    own_out,
    recv_bulk,
    recv_stat,
    rew,
    val,
    end,
    time_rew,
    time_val,
    time_end,
    time_r,
    time_a,
    time_m,
    send_bulk,
    send_z,
    recv_z,
    send_stat,
    in_sem,
    bulk_ss,
    bulk_rs,
    z_ss,
    z_rs,
    stat_ss,
    stat_rs,
    ready_sem,
):
    height, span = rew.shape
    count = span // LANES
    chunks = 4
    chunk_cols = span // chunks
    tm = lax.axis_index("tm")
    me = lax.axis_index("batch")
    core = lax.rem(tm, 2)
    partner = tm + 1 - 2 * core
    start = tm * span

    def loads(k):
        cols = pl.ds(k * chunk_cols, chunk_cols)
        return [
            pltpu.make_async_copy(source.at[:, cols], target.at[:, cols], in_sem.at[k, n])
            for n, (source, target) in enumerate(((rew_hbm, rew), (val_hbm, val), (end_hbm, end)))
        ]

    for k in range(chunks):
        for copy in loads(k):
            copy.start()

    barrier = pltpu.get_barrier_semaphore()
    for d in range(1, n_batch):
        pl.semaphore_signal(
            barrier,
            inc=1,
            device_id={"tm": tm - core, "batch": lax.rem(me + d, n_batch)},
            device_id_type=MESH,
        )
    for d in range(1, n_tm // 2):
        pl.semaphore_signal(
            barrier,
            inc=1,
            device_id={"tm": lax.rem(tm - core + 2 * d, n_tm) + 1, "batch": me},
            device_id_type=MESH,
        )
    pl.semaphore_signal(
        barrier, inc=1, device_id={"tm": partner, "batch": me}, device_id_type=MESH
    )

    lengths_row = len_ref[...]

    for k in range(chunks):
        for copy in loads(k):
            copy.wait()
        for j in range(k * (count // chunks), (k + 1) * (count // chunks)):
            rows = pl.ds(j * STRIDE, LANES)
            for source, target in ((rew, time_rew), (val, time_val), (end, time_end)):
                target[rows, :] = source[:, j * LANES : (j + 1) * LANES].T

    sublane = lax.broadcasted_iota(jnp.int32, (TILE, LANES), 0)
    lengths = jnp.broadcast_to(lengths_row, (TILE, LANES))
    limit = lengths - (start + sublane * LANES)
    rate = second_rate(lengths.astype(F32))
    whole_seg_a = squarings(rate, 7)[7]
    whole_seg_r = GAMMA_RATE**LANES

    def terms(k, value_next):
        at = pl.ds(k, TILE, stride=STRIDE)
        reward, value, ends = time_rew[at, :], time_val[at, :], time_end[at, :]
        inside = k < limit
        carry_on = (k < limit - 1) & (ends != 1)
        reward_in = jnp.where(inside, reward, 0.0)
        follow = jnp.where(carry_on, GAMMA_RATE * value_next, 0.0)
        delta = jnp.where(inside, reward_in + follow - value, 0.0)
        return at, value, carry_on, reward_in, delta

    def heads(step, carried):
        value_next, sum_r, sum_a, whole = carried
        _, value, carry_on, reward_in, delta = terms(LANES - 1 - step, value_next)
        sum_r = reward_in + jnp.where(carry_on, GAMMA_RATE * sum_r, 0.0)
        sum_a = delta + jnp.where(carry_on, rate * sum_a, 0.0)
        return value, sum_r, sum_a, jnp.where(carry_on, whole, 0.0)

    nought = limit.astype(F32) * 0.0
    first_value, head_r, head_a, whole = lax.fori_loop(
        0, LANES, heads, (nought, nought, nought, nought + 1.0), unroll=8
    )
    head_a = head_a + first_value * (GAMMA_RATE / rate)
    into_r = into_a = nought
    into_m = jnp.where(sublane == TILE - 1, 1.0, nought)
    for _ in range(TILE - 1):
        into_r = head_r + whole * whole_seg_r * into_r
        into_a = head_a + whole * whole_seg_a * into_a
        into_m = whole * whole_seg_a * into_m
        last = sublane == TILE - 1
        into_r = jnp.where(last, 0.0, pltpu.roll(into_r, TILE - 1, 0))
        into_a = jnp.where(last, 0.0, pltpu.roll(into_a, TILE - 1, 0))
        into_m = jnp.where(last, 1.0, pltpu.roll(into_m, TILE - 1, 0))

    def scan(step, carried):
        value_next, sum_r, sum_a, tail, totals = carried
        at, value, carry_on, reward_in, delta = terms(LANES - 1 - step, value_next)
        sum_r = reward_in + jnp.where(carry_on, GAMMA_RATE * sum_r, 0.0)
        sum_a = delta + jnp.where(carry_on, rate * sum_a, 0.0)
        tail = jnp.where(carry_on, rate * tail, 0.0)
        time_r[at, :] = sum_r
        time_a[at, :] = sum_a
        time_m[at, :] = tail
        more = (jnp.where(tail > 0.0, 1.0, 0.0), sum_a, sum_a * sum_a, sum_a * tail, tail, tail * tail)
        return value, sum_r, sum_a, tail, tuple(t + m for t, m in zip(totals, more))

    _, head_r, head_a, _, totals = lax.fori_loop(
        0, LANES, scan, (nought, into_r, into_a, into_m, (nought,) * 6), unroll=8
    )
    head_a = head_a + first_value * (GAMMA_RATE / rate)
    send_z[...] = jnp.concatenate(
        [head_r[:1], head_a[:1]] + [jnp.sum(total, axis=0, keepdims=True) for total in totals],
        axis=0,
    )
    recv_z[tm] = send_z[...]

    order = lax.broadcasted_iota(jnp.int32, (height, height), 0) == jnp.broadcast_to(
        grp_ref[...], (height, height)
    )
    order = jnp.where(order, 1.0, 0.0).astype(BF16)
    twice = jnp.concatenate([order, order], axis=1)
    thrice = jnp.concatenate([order, order, order], axis=1)
    wide = 2 * LANES

    def permute(c, _):
        cols = pl.ds(pl.multiple_of(c * wide, wide), wide)
        for n, source in enumerate((time_r, time_a)):
            parts = [
                source[pl.ds(pl.multiple_of((2 * c + h) * STRIDE, TILE), LANES), :] for h in (0, 1)
            ]
            pieces = jnp.concatenate(split(jnp.concatenate(parts, axis=0), 2), axis=1)
            moved = lax.dot_general(
                twice, pieces, (((1,), (1,)), ((), ())), preferred_element_type=F32
            )
            send_bulk[:, n * TILE : (n + 1) * TILE, cols] = moved.reshape(n_batch, TILE, wide)
        return 0


    @pl.when(core == 0)
    def _():
        pl.semaphore_wait(barrier, 2 * n_batch - 1)
        pl.semaphore_signal(
            ready_sem, inc=1, device_id={"tm": partner, "batch": me}, device_id_type=MESH
        )

    @pl.when(core == 1)
    def _():
        pl.semaphore_wait(ready_sem, 1)

    def bulk(to, slot):
        return pltpu.make_async_remote_copy(
            src_ref=send_bulk.at[to],
            dst_ref=recv_bulk.at[slot],
            send_sem=bulk_ss.at[to],
            recv_sem=bulk_rs.at[slot],
            device_id={"tm": tm, "batch": to},
            device_id_type=MESH,
        )

    def send_one(d, _):
        bulk(lax.rem(me + d, n_batch), me).start()
        return 0

    def send_all():
        lax.fori_loop(0, span // wide, permute, 0)
        lax.fori_loop(1, n_batch, send_one, 0)

    @pl.when(tm < n_tm // 2)
    def _():
        send_all()

    @pl.when(core == 1)
    def _():
        pl.semaphore_wait(barrier, n_tm - 1)
        pl.semaphore_signal(
            ready_sem, inc=1, device_id={"tm": partner, "batch": me}, device_id_type=MESH
        )

    @pl.when(core == 0)
    def _():
        pl.semaphore_wait(ready_sem, 1)

    def along(to, slot):
        return pltpu.make_async_remote_copy(
            src_ref=send_z,
            dst_ref=recv_z.at[slot],
            send_sem=z_ss.at[to],
            recv_sem=z_rs.at[slot],
            device_id={"tm": to, "batch": me},
            device_id_type=MESH,
        )

    def tell_one(d, _):
        along(lax.rem(tm + d, n_tm), tm).start()
        return 0

    lax.fori_loop(1, n_tm, tell_one, 0)
    @pl.when(tm >= n_tm // 2)
    def _():
        send_all()

    recv_bulk[me] = send_bulk[me]

    def hear_one(d, _):
        along(lax.rem(tm + d, n_tm), lax.rem(tm + d, n_tm)).wait_recv()
        return 0

    lax.fori_loop(1, n_tm, hear_one, 0)

    lengths_f = lengths_row.astype(F32)
    whole_a = squarings(second_rate(lengths_f), 10)[10]
    whole_r = GAMMA_RATE**span
    whole_a = jnp.broadcast_to(whole_a, (TILE, LANES))
    zero = whole_a * 0.0

    def chain(k, carried):
        block = n_tm - 1 - k
        into_r, into_a, own_r, own_a, first, second = carried
        tile = recv_z[block]
        piece = [jnp.broadcast_to(tile[n : n + 1], (TILE, LANES)) for n in range(TILE)]
        mine = jnp.where(block == tm, 1.0, 0.0)
        own_r = own_r + mine * into_r
        own_a = own_a + mine * into_a
        first = first + piece[3] + piece[6] * into_a
        second = second + piece[4] + into_a * (2.0 * piece[5] + piece[7] * into_a)
        whole = piece[2] == float(span)
        into_r = piece[0] + jnp.where(whole, whole_r, 0.0) * into_r
        into_a = piece[1] + jnp.where(whole, whole_a, 0.0) * into_a
        return into_r, into_a, own_r, own_a, first, second

    _, _, own_r, own_a, first, second = lax.fori_loop(0, n_tm, chain, (zero,) * 6)
    lines = jnp.concatenate(
        [line[:1] for line in (own_r, own_a, first, second, send_z[2:3], lengths_f)]
        + [lengths_f - start.astype(F32), jnp.zeros((height - 7, LANES), F32)],
        axis=0,
    )
    send_stat[...] = lax.dot_general(
        thrice,
        jnp.concatenate(split(lines, 3), axis=1),
        (((1,), (1,)), ((), ())),
        preferred_element_type=F32,
    )
    recv_stat[me] = send_stat[pl.ds(pl.multiple_of(me * TILE, TILE), TILE), :]

    def stat(to, slot):
        return pltpu.make_async_remote_copy(
            src_ref=send_stat.at[pl.ds(pl.multiple_of(to * TILE, TILE), TILE), :],
            dst_ref=recv_stat.at[slot],
            send_sem=stat_ss.at[to],
            recv_sem=stat_rs.at[slot],
            device_id={"tm": tm, "batch": to},
            device_id_type=MESH,
        )

    def send_stats(d, _):
        stat(lax.rem(me + d, n_batch), me).start()
        return 0

    lax.fori_loop(1, n_batch, send_stats, 0)

    own_into = jnp.broadcast_to(own_a[:1], (LANES, LANES))
    for j in range(count):
        rows = pl.ds(j * STRIDE, LANES)
        own_out[:, j * LANES : (j + 1) * LANES] = (time_a[rows, :] + time_m[rows, :] * own_into).T
    def hear_stats(d, _):
        slot = lax.rem(me + d, n_batch)
        stat(slot, slot).wait_recv()
        return 0

    lax.fori_loop(1, n_batch, hear_stats, 0)
    def sent(d, _):
        to = lax.rem(me + d, n_batch)
        bulk(to, to).wait_recv()
        bulk(to, me).wait_send()
        stat(to, me).wait_send()
        return 0

    lax.fori_loop(1, n_batch, sent, 0)

    def told(d, _):
        along(lax.rem(tm + d, n_tm), tm).wait_send()
        return 0

    lax.fori_loop(1, n_tm, told, 0)


def finish(own, bulk, stats, adv_out, gadv_out, gret_out, held, done_r, done_a, out_sem):
    n_batch = bulk.shape[0]
    span = bulk.shape[2]
    count = span // LANES
    own_copy = pltpu.make_async_copy(own, adv_out, out_sem.at[0])
    own_copy.start()
    total = stats[0]
    for i in range(1, n_batch):
        total = total + stats[i]
    counted = total[:, 5:6]
    mean = total[:, 2:3] / counted
    var = total[:, 3:4] / counted - mean * mean
    mean = jnp.broadcast_to(mean, (TILE, LANES))
    inverse = jnp.broadcast_to(1.0 / jnp.sqrt(var + EPSILON), (TILE, LANES))
    lane = lax.broadcasted_iota(jnp.int32, (TILE, LANES), 1)
    lane_f = lane.astype(F32)
    gamma_powers = [GAMMA_RATE ** (1 << bit) for bit in range(8)]
    for i in range(n_batch):
        facts = stats[i]
        into_r, into_a, opened, lengths, limit = [
            jnp.broadcast_to(facts[:, n : n + 1], (TILE, LANES)) for n in (0, 1, 4, 5, 6)
        ]
        powers = squarings(second_rate(lengths), 7)
        scale = powers[7] / lane_powers(powers[:7], lane)
        held[0, i] = into_r
        held[1, i] = into_a * scale
        held[2, i] = powers[7]
        held[3, i] = float(span - 1) - opened
        held[4, i] = limit

    def stores(j):
        cols = pl.ds(pl.multiple_of(j * LANES, LANES), LANES)
        return [
            pltpu.make_async_copy(source.at[j], target.at[:, cols], out_sem.at[1 + 2 * j + n])
            for n, (source, target) in enumerate(((done_r, gret_out), (done_a, gadv_out)))
        ]

    def column(step, scale_r):
        j = count - 1 - step
        cols = pl.ds(pl.multiple_of(j * LANES, LANES), LANES)
        place = lane_f + (j * LANES).astype(F32)
        for i in range(n_batch):
            carried = place > held[3, i]
            more = held[1, i]
            ret = bulk[i, :TILE, cols] + jnp.where(carried, scale_r, 0.0) * held[0, i]
            adv = bulk[i, TILE:, cols] + jnp.where(carried, more, 0.0)
            held[1, i] = more * held[2, i]
            rows = pl.ds(i, TILE, stride=n_batch)
            done_r[j, rows, :] = ret
            done_a[j, rows, :] = jnp.where(place < held[4, i], (adv - mean) * inverse, 0.0)
        for copy in stores(j):
            copy.start()
        return scale_r * gamma_powers[7]

    lax.fori_loop(0, count, column, gamma_powers[7] / lane_powers(gamma_powers[:7], lane))
    own_copy.wait()
    for j in range(count):
        for copy in stores(j):
            copy.wait()


def solution(mesh):
    n_tm, n_batch = mesh.shape["tm"], mesh.shape["batch"]

    def on_device(rewards, values, episode_ends, lengths, groups):
        height, span = rewards.shape
        block = pltpu.VMEM((height, span), F32)
        square = pltpu.VMEM((height, LANES), F32)
        turned = pltpu.VMEM((TILE * STRIDE, LANES), F32)
        out = jax.ShapeDtypeStruct((height, span), F32)

        def kernel(*refs):
            fused(n_tm, n_batch, *refs)

        own, bulk, stats = pl.pallas_call(
            kernel,
            out_shape=(
                pltpu.VMEM((height, span), F32),
                pltpu.VMEM((n_batch, 2 * TILE, span), F32),
                pltpu.VMEM((n_batch, TILE, LANES), F32),
            ),
            in_specs=[pl.BlockSpec(memory_space=pltpu.VMEM)] * 2
            + [pl.BlockSpec(memory_space=pl.ANY)] * 3,
            out_specs=[pl.BlockSpec(memory_space=pltpu.VMEM)] * 3,
            scratch_shapes=[
                block,
                block,
                pltpu.VMEM((height, span), jnp.int32),
                turned,
                turned,
                pltpu.VMEM((TILE * STRIDE, LANES), jnp.int32),
                turned,
                turned,
                turned,
                pltpu.VMEM((n_batch, 2 * TILE, span), F32),
                pltpu.VMEM((TILE, LANES), F32),
                pltpu.VMEM((n_tm, TILE, LANES), F32),
                square,
                pltpu.SemaphoreType.DMA((4, 3)),
                pltpu.SemaphoreType.DMA((n_batch,)),
                pltpu.SemaphoreType.DMA((n_batch,)),
                pltpu.SemaphoreType.DMA((n_tm,)),
                pltpu.SemaphoreType.DMA((n_tm,)),
                pltpu.SemaphoreType.DMA((n_batch,)),
                pltpu.SemaphoreType.DMA((n_batch,)),
                pltpu.SemaphoreType.REGULAR,
            ],
            compiler_params=pltpu.CompilerParams(collective_id=0, has_side_effects=True),
        )(lengths.reshape(1, height), groups.reshape(1, height), rewards, values, episode_ends)
        columns = pltpu.VMEM((span // LANES, height, LANES), F32)
        return pl.pallas_call(
            finish,
            out_shape=(out, out, out),
            in_specs=[pl.BlockSpec(memory_space=pltpu.VMEM)] * 3,
            out_specs=[pl.BlockSpec(memory_space=pl.ANY)] * 3,
            scratch_shapes=[
                pltpu.VMEM((5, n_batch, TILE, LANES), F32),
                columns,
                columns,
                pltpu.SemaphoreType.DMA((1 + 2 * (span // LANES),)),
            ],
        )(*[pltpu.with_memory_space_constraint(a, pltpu.VMEM) for a in (own, bulk, stats)])

    return jax.shard_map(
        on_device,
        mesh=mesh,
        in_specs=(
            P("batch", "tm"),
            P("batch", "tm"),
            P("batch", "tm"),
            P("batch"),
            P("batch"),
        ),
        out_specs=(P("batch", "tm"), P("batch", "tm"), P("batch", "tm")),
        check_vma=False,
    )
```

```python
import math

import jax
import jax.numpy as jnp
from jax import lax
from jax.experimental import pallas as pl
from jax.experimental.pallas import tpu as pltpu
from jax.sharding import PartitionSpec as P

MESH = pl.DeviceIdType.MESH
F32 = jnp.float32
BF16 = jnp.bfloat16
GAMMA_RATE = 0.9995
ALPHA_RATE = 0.05
EPSILON = 1e-06
LANES = 128
TILE = 8
STRIDE = 136


def second_rate(lengths):
    return GAMMA_RATE * (1.0 - 1.0 / (ALPHA_RATE * lengths))


def squarings(rate, count):
    powers = [rate]
    for _ in range(count):
        powers.append(powers[-1] * powers[-1])
    return powers


def lane_powers(powers, exponent):
    result = None
    for bit, power in enumerate(powers):
        factor = jnp.where((exponent & (1 << bit)) != 0, power, 1.0)
        result = factor if result is None else result * factor
    return result


def split(value, terms):
    pieces = []
    for _ in range(terms):
        piece = value.astype(BF16)
        pieces.append(piece)
        value = value - piece.astype(F32)
    return pieces


def fused(
    n_tm,
    n_batch,
    len_hbm,
    grp_hbm,
    rew_hbm,
    val_hbm,
    end_hbm,
    own_out,
    recv_bulk,
    recv_stat,
    len_ref,
    grp_ref,
    rew,
    val,
    end,
    time_rew,
    time_val,
    time_end,
    time_r,
    time_a,
    time_m,
    send_bulk,
    send_z,
    recv_z,
    send_stat,
    send_pair,
    recv_pair,
    in_sem,
    small_sem,
    pair_ss,
    pair_rs,
    bulk_ss,
    bulk_rs,
    z_ss,
    z_rs,
    stat_ss,
    stat_rs,
    ready_sem,
):
    height, span = rew.shape
    count = span // LANES
    chunks = 4
    chunk_cols = span // chunks
    tm = lax.axis_index("tm")
    me = lax.axis_index("batch")
    core = lax.rem(tm, 2)
    partner = tm + 1 - 2 * core
    start = tm * span
    chip = lax.div(tm, 2)
    n_chips = n_tm // 2
    side = math.isqrt(n_batch)
    row, column = lax.div(me, side), lax.rem(me, side)

    def away(distance, around):
        return min(distance, around - distance)

    steps = [(dx, dy) for dx in range(side) for dy in range(side) if dx or dy]
    steps.sort(key=lambda step: -away(step[0], side) - away(step[1], side))
    others = [lax.rem(row + dx, side) * side + lax.rem(column + dy, side) for dx, dy in steps]
    chip_steps = sorted(range(1, n_chips), key=lambda step: -away(step, n_chips))

    def loads(k):
        cols = pl.ds(k * chunk_cols, chunk_cols)
        return [
            pltpu.make_async_copy(source.at[:, cols], target.at[:, cols], in_sem.at[k, n])
            for n, (source, target) in enumerate(((rew_hbm, rew), (val_hbm, val), (end_hbm, end)))
        ]

    small = [
        pltpu.make_async_copy(source, target, small_sem.at[n])
        for n, (source, target) in enumerate(((len_hbm, len_ref), (grp_hbm, grp_ref)))
    ]
    for k in range(chunks):
        for copy in loads(k):
            copy.start()
    for copy in small:
        copy.start()

    barrier = pltpu.get_barrier_semaphore()
    for d in range(1, n_batch):
        pl.semaphore_signal(
            barrier,
            inc=1,
            device_id={"tm": tm - core, "batch": lax.rem(me + d, n_batch)},
            device_id_type=MESH,
        )
    for d in range(1, n_tm // 2):
        pl.semaphore_signal(
            barrier,
            inc=1,
            device_id={"tm": lax.rem(tm - core + 2 * d, n_tm) + 1, "batch": me},
            device_id_type=MESH,
        )
    pl.semaphore_signal(
        barrier, inc=1, device_id={"tm": partner, "batch": me}, device_id_type=MESH
    )

    for k in range(chunks):
        for copy in loads(k):
            copy.wait()
        for j in range(k * (count // chunks), (k + 1) * (count // chunks)):
            rows = pl.ds(j * STRIDE, LANES)
            for source, target in ((rew, time_rew), (val, time_val), (end, time_end)):
                target[rows, :] = source[:, j * LANES : (j + 1) * LANES].T

    for copy in small:
        copy.wait()
    lengths_row = len_ref[...]
    sublane = lax.broadcasted_iota(jnp.int32, (TILE, LANES), 0)
    lengths = jnp.broadcast_to(lengths_row, (TILE, LANES))
    limit = lengths - (start + sublane * LANES)
    rate = second_rate(lengths.astype(F32))
    whole_seg_a = squarings(rate, 7)[7]
    whole_seg_r = GAMMA_RATE**LANES

    def terms(k, value_next):
        at = pl.ds(k, TILE, stride=STRIDE)
        reward, value, ends = time_rew[at, :], time_val[at, :], time_end[at, :]
        inside = k < limit
        carry_on = (k < limit - 1) & (ends != 1)
        reward_in = jnp.where(inside, reward, 0.0)
        follow = jnp.where(carry_on, GAMMA_RATE * value_next, 0.0)
        delta = jnp.where(inside, reward_in + follow - value, 0.0)
        return at, value, carry_on, reward_in, delta

    def heads(step, carried):
        value_next, sum_r, sum_a, whole = carried
        _, value, carry_on, reward_in, delta = terms(LANES - 1 - step, value_next)
        sum_r = reward_in + jnp.where(carry_on, GAMMA_RATE * sum_r, 0.0)
        sum_a = delta + jnp.where(carry_on, rate * sum_a, 0.0)
        return value, sum_r, sum_a, jnp.where(carry_on, whole, 0.0)

    nought = limit.astype(F32) * 0.0
    first_value, head_r, head_a, whole = lax.fori_loop(
        0, LANES, heads, (nought, nought, nought, nought + 1.0), unroll=8
    )
    head_a = head_a + first_value * (GAMMA_RATE / rate)
    into_r = into_a = nought
    into_m = jnp.where(sublane == TILE - 1, 1.0, nought)
    for _ in range(TILE - 1):
        into_r = head_r + whole * whole_seg_r * into_r
        into_a = head_a + whole * whole_seg_a * into_a
        into_m = whole * whole_seg_a * into_m
        last = sublane == TILE - 1
        into_r = jnp.where(last, 0.0, pltpu.roll(into_r, TILE - 1, 0))
        into_a = jnp.where(last, 0.0, pltpu.roll(into_a, TILE - 1, 0))
        into_m = jnp.where(last, 1.0, pltpu.roll(into_m, TILE - 1, 0))

    def scan(step, carried):
        value_next, sum_r, sum_a, tail, totals = carried
        at, value, carry_on, reward_in, delta = terms(LANES - 1 - step, value_next)
        sum_r = reward_in + jnp.where(carry_on, GAMMA_RATE * sum_r, 0.0)
        sum_a = delta + jnp.where(carry_on, rate * sum_a, 0.0)
        tail = jnp.where(carry_on, rate * tail, 0.0)
        time_r[at, :] = sum_r
        time_a[at, :] = sum_a
        time_m[at, :] = tail
        more = (jnp.where(tail > 0.0, 1.0, 0.0), sum_a, sum_a * sum_a, sum_a * tail, tail, tail * tail)
        return value, sum_r, sum_a, tail, tuple(t + m for t, m in zip(totals, more))

    _, head_r, head_a, _, totals = lax.fori_loop(
        0, LANES, scan, (nought, into_r, into_a, into_m, (nought,) * 6), unroll=8
    )
    head_a = head_a + first_value * (GAMMA_RATE / rate)
    send_z[...] = jnp.concatenate(
        [head_r[:1], head_a[:1]] + [jnp.sum(total, axis=0, keepdims=True) for total in totals],
        axis=0,
    )

    order = lax.broadcasted_iota(jnp.int32, (height, height), 0) == jnp.broadcast_to(
        grp_ref[...], (height, height)
    )
    order = jnp.where(order, 1.0, 0.0).astype(BF16)
    twice = jnp.concatenate([order, order], axis=1)
    thrice = jnp.concatenate([order, order, order], axis=1)
    wide = 2 * LANES

    def permute(c, _):
        cols = pl.ds(pl.multiple_of(c * wide, wide), wide)
        for n, source in enumerate((time_r, time_a)):
            parts = [
                source[pl.ds(pl.multiple_of((2 * c + h) * STRIDE, TILE), LANES), :] for h in (0, 1)
            ]
            pieces = jnp.concatenate(split(jnp.concatenate(parts, axis=0), 2), axis=1)
            moved = lax.dot_general(
                twice, pieces, (((1,), (1,)), ((), ())), preferred_element_type=F32
            )
            send_bulk[:, n * TILE : (n + 1) * TILE, cols] = moved.reshape(n_batch, TILE, wide)
        return 0


    @pl.when(core == 0)
    def _():
        pl.semaphore_wait(barrier, 2 * n_batch - 1)
        pl.semaphore_signal(
            ready_sem, inc=1, device_id={"tm": partner, "batch": me}, device_id_type=MESH
        )

    @pl.when(core == 1)
    def _():
        pl.semaphore_wait(ready_sem, 1)

    def bulk(to, slot):
        return pltpu.make_async_remote_copy(
            src_ref=send_bulk.at[to],
            dst_ref=recv_bulk.at[slot],
            send_sem=bulk_ss.at[to],
            recv_sem=bulk_rs.at[slot],
            device_id={"tm": tm, "batch": to},
            device_id_type=MESH,
        )

    def send_all():
        for to in others:
            bulk(to, me).start()

    pair = pltpu.make_async_remote_copy(
        src_ref=send_z,
        dst_ref=recv_pair,
        send_sem=pair_ss,
        recv_sem=pair_rs,
        device_id={"tm": partner, "batch": me},
        device_id_type=MESH,
    )
    pair.start()
    lax.fori_loop(0, span // wide, permute, 0)

    @pl.when(tm < n_tm // 2)
    def _():
        send_all()

    pair.wait()
    lengths_f = lengths_row.astype(F32)
    whole_a = jnp.broadcast_to(squarings(second_rate(lengths_f), 10)[10], (TILE, LANES))
    whole_r = GAMMA_RATE**span
    mine, theirs = send_z[...], recv_pair[...]

    def pieces_of(tile):
        return [jnp.broadcast_to(tile[n : n + 1], (TILE, LANES)) for n in range(TILE)]

    early = pieces_of(jnp.where(core == 0, mine, theirs))
    late = pieces_of(jnp.where(core == 0, theirs, mine))
    early_open = jnp.where(early[2] == float(span), 1.0, 0.0)
    late_open = jnp.where(late[2] == float(span), 1.0, 0.0)
    late_r, late_a = late_open * whole_r, late_open * whole_a
    joined = (
        early[0] + early_open * whole_r * late[0],
        early[1] + early_open * whole_a * late[1],
        early_open * late_open,
        late[3] + early[3] + early[6] * late[1],
        late[4] + early[4] + late[1] * (2.0 * early[5] + early[7] * late[1]),
        late[5] + late_a * (early[5] + early[7] * late[1]),
        late[6] + early[6] * late_a,
        late[7] + early[7] * late_a * late_a,
    )
    send_pair[...] = jnp.concatenate([line[:1] for line in joined], axis=0)
    recv_z[chip] = send_pair[...]

    @pl.when(core == 1)
    def _():
        pl.semaphore_wait(barrier, n_tm - 1)
        pl.semaphore_signal(
            ready_sem, inc=1, device_id={"tm": partner, "batch": me}, device_id_type=MESH
        )

    @pl.when(core == 0)
    def _():
        pl.semaphore_wait(ready_sem, 1)

    def along(to, slot):
        return pltpu.make_async_remote_copy(
            src_ref=send_pair,
            dst_ref=recv_z.at[slot],
            send_sem=z_ss.at[to],
            recv_sem=z_rs.at[slot],
            device_id={"tm": 2 * to + core, "batch": me},
            device_id_type=MESH,
        )

    for step in chip_steps:
        along(lax.rem(chip + step, n_chips), chip).start()

    @pl.when(tm >= n_tm // 2)
    def _():
        send_all()

    recv_bulk[me] = send_bulk[me]

    def hear_one(d, _):
        other = lax.rem(chip + d, n_chips)
        along(other, other).wait_recv()
        return 0

    lax.fori_loop(1, n_chips, hear_one, 0)

    both_r, both_a = whole_r * whole_r, whole_a * whole_a
    zero = whole_a * 0.0

    def chain(k, carried):
        block = n_chips - 1 - k
        into_r, into_a, own_r, own_a, first, second = carried
        piece = pieces_of(recv_z[block])
        here = jnp.where(block == chip, 1.0, 0.0)
        own_r = own_r + here * into_r
        own_a = own_a + here * into_a
        first = first + piece[3] + piece[6] * into_a
        second = second + piece[4] + into_a * (2.0 * piece[5] + piece[7] * into_a)
        into_r = piece[0] + piece[2] * both_r * into_r
        into_a = piece[1] + piece[2] * both_a * into_a
        return into_r, into_a, own_r, own_a, first, second

    _, _, own_r, own_a, first, second = lax.fori_loop(0, n_chips, chain, (zero,) * 6, unroll=4)
    is_early = jnp.where(core == 0, 1.0, 0.0)
    own_r = is_early * (late[0] + late_r * own_r) + (1.0 - is_early) * own_r
    own_a = is_early * (late[1] + late_a * own_a) + (1.0 - is_early) * own_a
    lines = jnp.concatenate(
        [line[:1] for line in (own_r, own_a, first, second, send_z[2:3], lengths_f)]
        + [lengths_f - start.astype(F32), jnp.zeros((height - 7, LANES), F32)],
        axis=0,
    )
    send_stat[...] = lax.dot_general(
        thrice,
        jnp.concatenate(split(lines, 3), axis=1),
        (((1,), (1,)), ((), ())),
        preferred_element_type=F32,
    )
    recv_stat[me] = send_stat[pl.ds(pl.multiple_of(me * TILE, TILE), TILE), :]

    def stat(to, slot):
        return pltpu.make_async_remote_copy(
            src_ref=send_stat.at[pl.ds(pl.multiple_of(to * TILE, TILE), TILE), :],
            dst_ref=recv_stat.at[slot],
            send_sem=stat_ss.at[to],
            recv_sem=stat_rs.at[slot],
            device_id={"tm": tm, "batch": to},
            device_id_type=MESH,
        )

    for to in others:
        stat(to, me).start()

    own_into = jnp.broadcast_to(own_a[:1], (LANES, LANES))
    for j in range(count):
        rows = pl.ds(j * STRIDE, LANES)
        own_out[:, j * LANES : (j + 1) * LANES] = (time_a[rows, :] + time_m[rows, :] * own_into).T
    def hear_stats(d, _):
        slot = lax.rem(me + d, n_batch)
        stat(slot, slot).wait_recv()
        return 0

    lax.fori_loop(1, n_batch, hear_stats, 0)
    def sent(d, _):
        to = lax.rem(me + d, n_batch)
        bulk(to, to).wait_recv()
        bulk(to, me).wait_send()
        stat(to, me).wait_send()
        return 0

    lax.fori_loop(1, n_batch, sent, 0)

    def told(d, _):
        along(lax.rem(chip + d, n_chips), chip).wait_send()
        return 0

    lax.fori_loop(1, n_chips, told, 0)


def finish(own, bulk, stats, adv_out, gadv_out, gret_out, held, done_r, done_a, out_sem):
    n_batch = bulk.shape[0]
    span = bulk.shape[2]
    count = span // LANES
    own_copy = pltpu.make_async_copy(own, adv_out, out_sem.at[0])
    own_copy.start()
    total = stats[0]
    for i in range(1, n_batch):
        total = total + stats[i]
    counted = total[:, 5:6]
    mean = total[:, 2:3] / counted
    var = total[:, 3:4] / counted - mean * mean
    mean = jnp.broadcast_to(mean, (TILE, LANES))
    inverse = jnp.broadcast_to(1.0 / jnp.sqrt(var + EPSILON), (TILE, LANES))
    lane = lax.broadcasted_iota(jnp.int32, (TILE, LANES), 1)
    lane_f = lane.astype(F32)
    gamma_powers = [GAMMA_RATE ** (1 << bit) for bit in range(8)]
    for i in range(n_batch):
        facts = stats[i]
        into_r, into_a, opened, lengths, limit = [
            jnp.broadcast_to(facts[:, n : n + 1], (TILE, LANES)) for n in (0, 1, 4, 5, 6)
        ]
        powers = squarings(second_rate(lengths), 7)
        scale = powers[7] / lane_powers(powers[:7], lane)
        held[0, i] = into_r
        held[1, i] = into_a * scale
        held[2, i] = powers[7]
        held[3, i] = float(span - 1) - opened
        held[4, i] = limit

    def stores(j):
        cols = pl.ds(pl.multiple_of(j * LANES, LANES), LANES)
        return [
            pltpu.make_async_copy(source.at[j], target.at[:, cols], out_sem.at[1 + 2 * j + n])
            for n, (source, target) in enumerate(((done_r, gret_out), (done_a, gadv_out)))
        ]

    def column(step, scale_r):
        j = count - 1 - step
        cols = pl.ds(pl.multiple_of(j * LANES, LANES), LANES)
        place = lane_f + (j * LANES).astype(F32)
        for i in range(n_batch):
            carried = place > held[3, i]
            more = held[1, i]
            ret = bulk[i, :TILE, cols] + jnp.where(carried, scale_r, 0.0) * held[0, i]
            adv = bulk[i, TILE:, cols] + jnp.where(carried, more, 0.0)
            held[1, i] = more * held[2, i]
            rows = pl.ds(i, TILE, stride=n_batch)
            done_r[j, rows, :] = ret
            done_a[j, rows, :] = jnp.where(place < held[4, i], (adv - mean) * inverse, 0.0)
        for copy in stores(j):
            copy.start()
        return scale_r * gamma_powers[7]

    lax.fori_loop(0, count, column, gamma_powers[7] / lane_powers(gamma_powers[:7], lane))
    own_copy.wait()
    for j in range(count):
        for copy in stores(j):
            copy.wait()


def solution(mesh):
    n_tm, n_batch = mesh.shape["tm"], mesh.shape["batch"]

    def on_device(rewards, values, episode_ends, lengths, groups):
        height, span = rewards.shape
        block = pltpu.VMEM((height, span), F32)
        square = pltpu.VMEM((height, LANES), F32)
        turned = pltpu.VMEM((TILE * STRIDE, LANES), F32)
        out = jax.ShapeDtypeStruct((height, span), F32)

        def kernel(*refs):
            fused(n_tm, n_batch, *refs)

        own, bulk, stats = pl.pallas_call(
            kernel,
            out_shape=(
                pltpu.VMEM((height, span), F32),
                pltpu.VMEM((n_batch, 2 * TILE, span), F32),
                pltpu.VMEM((n_batch, TILE, LANES), F32),
            ),
            in_specs=[pl.BlockSpec(memory_space=pl.ANY)] * 5,
            out_specs=[pl.BlockSpec(memory_space=pltpu.VMEM)] * 3,
            scratch_shapes=[
                pltpu.VMEM((1, height), jnp.int32),
                pltpu.VMEM((1, height), jnp.int32),
                block,
                block,
                pltpu.VMEM((height, span), jnp.int32),
                turned,
                turned,
                pltpu.VMEM((TILE * STRIDE, LANES), jnp.int32),
                turned,
                turned,
                turned,
                pltpu.VMEM((n_batch, 2 * TILE, span), F32),
                pltpu.VMEM((TILE, LANES), F32),
                pltpu.VMEM((n_tm // 2, TILE, LANES), F32),
                square,
                pltpu.VMEM((TILE, LANES), F32),
                pltpu.VMEM((TILE, LANES), F32),
                pltpu.SemaphoreType.DMA((4, 3)),
                pltpu.SemaphoreType.DMA((2,)),
                pltpu.SemaphoreType.DMA,
                pltpu.SemaphoreType.DMA,
                pltpu.SemaphoreType.DMA((n_batch,)),
                pltpu.SemaphoreType.DMA((n_batch,)),
                pltpu.SemaphoreType.DMA((n_tm // 2,)),
                pltpu.SemaphoreType.DMA((n_tm // 2,)),
                pltpu.SemaphoreType.DMA((n_batch,)),
                pltpu.SemaphoreType.DMA((n_batch,)),
                pltpu.SemaphoreType.REGULAR,
            ],
            compiler_params=pltpu.CompilerParams(collective_id=0, has_side_effects=True),
        )(lengths.reshape(1, height), groups.reshape(1, height), rewards, values, episode_ends)
        columns = pltpu.VMEM((span // LANES, height, LANES), F32)
        return pl.pallas_call(
            finish,
            out_shape=(out, out, out),
            in_specs=[pl.BlockSpec(memory_space=pltpu.VMEM)] * 3,
            out_specs=[pl.BlockSpec(memory_space=pl.ANY)] * 3,
            scratch_shapes=[
                pltpu.VMEM((5, n_batch, TILE, LANES), F32),
                columns,
                columns,
                pltpu.SemaphoreType.DMA((1 + 2 * (span // LANES),)),
            ],
        )(*[pltpu.with_memory_space_constraint(a, pltpu.VMEM) for a in (own, bulk, stats)])

    return jax.shard_map(
        on_device,
        mesh=mesh,
        in_specs=(
            P("batch", "tm"),
            P("batch", "tm"),
            P("batch", "tm"),
            P("batch"),
            P("batch"),
        ),
        out_specs=(P("batch", "tm"), P("batch", "tm"), P("batch", "tm")),
        check_vma=False,
    )
```

```python
import math

import jax
import jax.numpy as jnp
from jax import lax
from jax.experimental import pallas as pl
from jax.experimental.pallas import tpu as pltpu
from jax.sharding import PartitionSpec as P

MESH = pl.DeviceIdType.MESH
F32 = jnp.float32
BF16 = jnp.bfloat16
GAMMA_RATE = 0.9995
ALPHA_RATE = 0.05
EPSILON = 1e-06
LANES = 128
TILE = 8
STRIDE = 136


def second_rate(lengths):
    return GAMMA_RATE * (1.0 - 1.0 / (ALPHA_RATE * lengths))


def squarings(rate, count):
    powers = [rate]
    for _ in range(count):
        powers.append(powers[-1] * powers[-1])
    return powers


def lane_powers(powers, exponent):
    result = None
    for bit, power in enumerate(powers):
        factor = jnp.where((exponent & (1 << bit)) != 0, power, 1.0)
        result = factor if result is None else result * factor
    return result


def joined(early, late):
    b_r, b_a, a_r, a_a, s_0, t_0, t_1, s_1, t_2 = early
    return [
        b_r + a_r * late[0],
        b_a + a_a * late[1],
        a_r * late[2],
        a_a * late[3],
        late[4] + s_0 + s_1 * late[1],
        late[5] + t_0 + late[1] * (2.0 * t_1 + t_2 * late[1]),
        late[6] + late[3] * (t_1 + t_2 * late[1]),
        late[7] + s_1 * late[3],
        late[8] + t_2 * late[3] * late[3],
    ]


def split(value, terms):
    pieces = []
    for _ in range(terms):
        piece = value.astype(BF16)
        pieces.append(piece)
        value = value - piece.astype(F32)
    return pieces


def fused(
    n_tm,
    n_batch,
    len_hbm,
    grp_hbm,
    rew_hbm,
    val_hbm,
    end_hbm,
    own_out,
    recv_bulk,
    recv_stat,
    len_ref,
    grp_ref,
    rew,
    val,
    end,
    time_rew,
    time_val,
    time_end,
    time_r,
    time_a,
    time_m,
    send_bulk,
    send_z,
    recv_z,
    send_stat,
    send_pair,
    recv_pair,
    in_sem,
    small_sem,
    pair_ss,
    pair_rs,
    bulk_ss,
    bulk_rs,
    z_ss,
    z_rs,
    stat_ss,
    stat_rs,
    ready_sem,
):
    height, span = rew.shape
    count = span // LANES
    chunks = 4
    chunk_cols = span // chunks
    tm = lax.axis_index("tm")
    me = lax.axis_index("batch")
    core = lax.rem(tm, 2)
    partner = tm + 1 - 2 * core
    start = tm * span
    chip = lax.div(tm, 2)
    n_chips = n_tm // 2
    side = math.isqrt(n_batch)
    row, column = lax.div(me, side), lax.rem(me, side)

    def away(distance, around):
        return min(distance, around - distance)

    steps = [(dx, dy) for dx in range(side) for dy in range(side) if dx or dy]
    steps.sort(key=lambda step: -away(step[0], side) - away(step[1], side))
    others = [lax.rem(row + dx, side) * side + lax.rem(column + dy, side) for dx, dy in steps]
    chip_steps = sorted(range(1, n_chips), key=lambda step: -away(step, n_chips))

    def loads(k):
        cols = pl.ds(k * chunk_cols, chunk_cols)
        return [
            pltpu.make_async_copy(source.at[:, cols], target.at[:, cols], in_sem.at[k, n])
            for n, (source, target) in enumerate(((rew_hbm, rew), (val_hbm, val), (end_hbm, end)))
        ]

    small = [
        pltpu.make_async_copy(source, target, small_sem.at[n])
        for n, (source, target) in enumerate(((len_hbm, len_ref), (grp_hbm, grp_ref)))
    ]
    for k in range(chunks):
        for copy in loads(k):
            copy.start()
    for copy in small:
        copy.start()

    barrier = pltpu.get_barrier_semaphore()
    for d in range(1, n_batch):
        pl.semaphore_signal(
            barrier,
            inc=1,
            device_id={"tm": tm - core, "batch": lax.rem(me + d, n_batch)},
            device_id_type=MESH,
        )
    for d in range(1, n_tm // 2):
        pl.semaphore_signal(
            barrier,
            inc=1,
            device_id={"tm": lax.rem(tm - core + 2 * d, n_tm) + 1, "batch": me},
            device_id_type=MESH,
        )
    pl.semaphore_signal(
        barrier, inc=1, device_id={"tm": partner, "batch": me}, device_id_type=MESH
    )

    for k in range(chunks):
        for copy in loads(k):
            copy.wait()
        for j in range(k * (count // chunks), (k + 1) * (count // chunks)):
            rows = pl.ds(j * STRIDE, LANES)
            for source, target in ((rew, time_rew), (val, time_val), (end, time_end)):
                target[rows, :] = source[:, j * LANES : (j + 1) * LANES].T

    for copy in small:
        copy.wait()
    lengths_row = len_ref[...]
    sublane = lax.broadcasted_iota(jnp.int32, (TILE, LANES), 0)
    lengths = jnp.broadcast_to(lengths_row, (TILE, LANES))
    limit = lengths - (start + sublane * LANES)
    rate = second_rate(lengths.astype(F32))
    whole_seg_a = squarings(rate, 7)[7]
    whole_seg_r = GAMMA_RATE**LANES

    def terms(k, value_next):
        at = pl.ds(k, TILE, stride=STRIDE)
        reward, value, ends = time_rew[at, :], time_val[at, :], time_end[at, :]
        inside = k < limit
        carry_on = (k < limit - 1) & (ends != 1)
        reward_in = jnp.where(inside, reward, 0.0)
        follow = jnp.where(carry_on, GAMMA_RATE * value_next, 0.0)
        delta = jnp.where(inside, reward_in + follow - value, 0.0)
        return at, value, carry_on, reward_in, delta

    def scan(step, carried):
        value_next, sum_r, sum_a, tail, totals = carried
        at, value, carry_on, reward_in, delta = terms(LANES - 1 - step, value_next)
        sum_r = reward_in + jnp.where(carry_on, GAMMA_RATE * sum_r, 0.0)
        sum_a = delta + jnp.where(carry_on, rate * sum_a, 0.0)
        tail = jnp.where(carry_on, rate * tail, 0.0)
        time_r[at, :] = sum_r
        time_a[at, :] = sum_a
        time_m[at, :] = tail
        more = (jnp.where(tail > 0.0, 1.0, 0.0), sum_a, sum_a * sum_a, sum_a * tail, tail, tail * tail)
        return value, sum_r, sum_a, tail, tuple(t + m for t, m in zip(totals, more))

    nought = limit.astype(F32) * 0.0
    first_value, head_r, head_a, _, totals = lax.fori_loop(
        0, LANES, scan, (nought, nought, nought, nought + 1.0, (nought,) * 6), unroll=8
    )
    head_a = head_a + first_value * (GAMMA_RATE / rate)
    seg_open = jnp.where(totals[0] == float(LANES), 1.0, 0.0)
    seg_r, seg_a = seg_open * whole_seg_r, seg_open * whole_seg_a
    tiles = (head_r, head_a, seg_r, seg_a) + totals[1:] + (totals[0], seg_open)
    done = None
    into_r = into_a = nought
    into_m = nought + 1.0
    for j in reversed(range(TILE)):
        segment = [jnp.broadcast_to(tile[j : j + 1], (TILE, LANES)) for tile in tiles]
        if done is None:
            done, opened, still_open = segment[:9], segment[9], segment[10]
            continue
        into_r = jnp.where(sublane == j, done[0], into_r)
        into_a = jnp.where(sublane == j, done[1], into_a)
        into_m = jnp.where(sublane == j, done[3], into_m)
        done = joined(segment[:9], done)
        opened = opened + still_open * segment[9]
        still_open = still_open * segment[10]
    send_z[...] = jnp.concatenate(
        [line[:1] for line in (done[0], done[1], opened, *done[4:])], axis=0
    )

    order = lax.broadcasted_iota(jnp.int32, (height, height), 0) == jnp.broadcast_to(
        grp_ref[...], (height, height)
    )
    order = jnp.where(order, 1.0, 0.0).astype(BF16)
    twice = jnp.concatenate([order, order], axis=1)
    thrice = jnp.concatenate([order, order, order], axis=1)
    wide = 2 * LANES

    def permute(c, _):
        cols = pl.ds(pl.multiple_of(c * wide, wide), wide)
        for n, source in enumerate((time_r, time_a)):
            parts = [
                source[pl.ds(pl.multiple_of((2 * c + h) * STRIDE, TILE), LANES), :] for h in (0, 1)
            ]
            pieces = jnp.concatenate(split(jnp.concatenate(parts, axis=0), 2), axis=1)
            moved = lax.dot_general(
                twice, pieces, (((1,), (1,)), ((), ())), preferred_element_type=F32
            )
            send_bulk[:, n * TILE : (n + 1) * TILE, cols] = moved.reshape(n_batch, TILE, wide)
        return 0


    @pl.when(core == 0)
    def _():
        pl.semaphore_wait(barrier, 2 * n_batch - 1)
        pl.semaphore_signal(
            ready_sem, inc=1, device_id={"tm": partner, "batch": me}, device_id_type=MESH
        )

    @pl.when(core == 1)
    def _():
        pl.semaphore_wait(ready_sem, 1)

    def bulk(to, slot):
        return pltpu.make_async_remote_copy(
            src_ref=send_bulk.at[to],
            dst_ref=recv_bulk.at[slot],
            send_sem=bulk_ss,
            recv_sem=bulk_rs,
            device_id={"tm": tm, "batch": to},
            device_id_type=MESH,
        )

    def send_all():
        left = LANES - lax.broadcasted_iota(jnp.int32, (LANES, LANES), 0)
        scale_r = lane_powers([GAMMA_RATE ** (1 << bit) for bit in range(8)], left)
        for j in range(TILE):
            rows = pl.ds(j * STRIDE, LANES)
            more_r, more_a, more_m = [
                jnp.broadcast_to(tile[j : j + 1], (LANES, LANES)) for tile in (into_r, into_a, into_m)
            ]
            tail = time_m[rows, :]
            time_r[rows, :] = time_r[rows, :] + jnp.where(tail > 0.0, scale_r, 0.0) * more_r
            time_a[rows, :] = time_a[rows, :] + tail * more_a
            time_m[rows, :] = tail * more_m
        lax.fori_loop(0, span // wide, permute, 0)
        for to in others:
            bulk(to, me).start()

    pair = pltpu.make_async_remote_copy(
        src_ref=send_z,
        dst_ref=recv_pair,
        send_sem=pair_ss,
        recv_sem=pair_rs,
        device_id={"tm": partner, "batch": me},
        device_id_type=MESH,
    )
    pair.start()


    @pl.when(tm < n_tm // 2)
    def _():
        send_all()

    @pl.when(core == 1)
    def _():
        pl.semaphore_wait(barrier, n_tm - 1)
        pl.semaphore_signal(
            ready_sem, inc=1, device_id={"tm": partner, "batch": me}, device_id_type=MESH
        )

    @pl.when(core == 0)
    def _():
        pl.semaphore_wait(ready_sem, 1)

    pair.wait()
    lengths_f = lengths_row.astype(F32)
    whole_a = jnp.broadcast_to(squarings(second_rate(lengths_f), 10)[10], (TILE, LANES))
    whole_r = GAMMA_RATE**span
    mine, theirs = send_z[...], recv_pair[...]

    def pieces_of(tile):
        return [jnp.broadcast_to(tile[n : n + 1], (TILE, LANES)) for n in range(TILE)]

    def block_of(tile):
        piece = pieces_of(tile)
        whole = jnp.where(piece[2] == float(span), 1.0, 0.0)
        return piece[:2] + [whole * whole_r, whole * whole_a] + piece[3:], whole

    early, early_open = block_of(jnp.where(core == 0, mine, theirs))
    late, late_open = block_of(jnp.where(core == 0, theirs, mine))
    both = joined(early, late)
    send_pair[...] = jnp.concatenate(
        [line[:1] for line in (both[0], both[1], early_open * late_open, *both[4:])], axis=0
    )
    recv_z[chip] = send_pair[...]

    def along(to, slot):
        return pltpu.make_async_remote_copy(
            src_ref=send_pair,
            dst_ref=recv_z.at[slot],
            send_sem=z_ss,
            recv_sem=z_rs,
            device_id={"tm": 2 * to + core, "batch": me},
            device_id_type=MESH,
        )

    for step in chip_steps:
        along(lax.rem(chip + step, n_chips), chip).start()

    @pl.when(tm >= n_tm // 2)
    def _():
        send_all()

    recv_bulk[me] = send_bulk[me]

    all_z = pltpu.make_async_remote_copy(
        src_ref=recv_z.at[pl.ds(0, n_chips - 1)],
        dst_ref=recv_z.at[pl.ds(0, n_chips - 1)],
        send_sem=z_ss,
        recv_sem=z_rs,
        device_id={"tm": partner, "batch": me},
        device_id_type=MESH,
    )
    all_z.wait_recv()

    both_r, both_a = whole_r * whole_r, whole_a * whole_a
    zero = whole_a * 0.0

    def chain(k, carried):
        block = n_chips - 1 - k
        into_r, into_a, own_r, own_a, first, second = carried
        piece = pieces_of(recv_z[block])
        here = jnp.where(block == chip, 1.0, 0.0)
        own_r = own_r + here * into_r
        own_a = own_a + here * into_a
        first = first + piece[3] + piece[6] * into_a
        second = second + piece[4] + into_a * (2.0 * piece[5] + piece[7] * into_a)
        into_r = piece[0] + piece[2] * both_r * into_r
        into_a = piece[1] + piece[2] * both_a * into_a
        return into_r, into_a, own_r, own_a, first, second

    _, _, own_r, own_a, first, second = lax.fori_loop(0, n_chips, chain, (zero,) * 6, unroll=4)
    is_early = jnp.where(core == 0, 1.0, 0.0)
    own_r = is_early * (late[0] + late[2] * own_r) + (1.0 - is_early) * own_r
    own_a = is_early * (late[1] + late[3] * own_a) + (1.0 - is_early) * own_a
    lines = jnp.concatenate(
        [line[:1] for line in (own_r, own_a, first, second, send_z[2:3], lengths_f)]
        + [lengths_f - start.astype(F32), jnp.zeros((height - 7, LANES), F32)],
        axis=0,
    )
    send_stat[...] = lax.dot_general(
        thrice,
        jnp.concatenate(split(lines, 3), axis=1),
        (((1,), (1,)), ((), ())),
        preferred_element_type=F32,
    )
    recv_stat[me] = send_stat[pl.ds(pl.multiple_of(me * TILE, TILE), TILE), :]

    def stat(to, slot):
        return pltpu.make_async_remote_copy(
            src_ref=send_stat.at[pl.ds(pl.multiple_of(to * TILE, TILE), TILE), :],
            dst_ref=recv_stat.at[slot],
            send_sem=stat_ss,
            recv_sem=stat_rs,
            device_id={"tm": tm, "batch": to},
            device_id_type=MESH,
        )

    for to in others:
        stat(to, me).start()

    own_into = jnp.broadcast_to(own_a[:1], (LANES, LANES))
    for j in range(count):
        rows = pl.ds(j * STRIDE, LANES)
        own_out[:, j * LANES : (j + 1) * LANES] = (time_a[rows, :] + time_m[rows, :] * own_into).T
    all_stats = pltpu.make_async_remote_copy(
        src_ref=recv_stat.at[pl.ds(0, n_batch - 1)],
        dst_ref=recv_stat.at[pl.ds(0, n_batch - 1)],
        send_sem=stat_ss,
        recv_sem=stat_rs,
        device_id={"tm": partner, "batch": me},
        device_id_type=MESH,
    )
    all_bulk = pltpu.make_async_remote_copy(
        src_ref=send_bulk.at[pl.ds(0, n_batch - 1)],
        dst_ref=recv_bulk.at[pl.ds(0, n_batch - 1)],
        send_sem=bulk_ss,
        recv_sem=bulk_rs,
        device_id={"tm": partner, "batch": me},
        device_id_type=MESH,
    )
    all_stats.wait()
    all_bulk.wait()
    all_z.wait_send()


def finish(own, bulk, stats, adv_out, gadv_out, gret_out, held, done_r, done_a, out_sem):
    n_batch = bulk.shape[0]
    span = bulk.shape[2]
    count = span // LANES
    own_copy = pltpu.make_async_copy(own, adv_out, out_sem.at[0])
    own_copy.start()
    total = stats[0]
    for i in range(1, n_batch):
        total = total + stats[i]
    counted = total[:, 5:6]
    mean = total[:, 2:3] / counted
    var = total[:, 3:4] / counted - mean * mean
    mean = jnp.broadcast_to(mean, (TILE, LANES))
    inverse = jnp.broadcast_to(1.0 / jnp.sqrt(var + EPSILON), (TILE, LANES))
    lane = lax.broadcasted_iota(jnp.int32, (TILE, LANES), 1)
    lane_f = lane.astype(F32)
    gamma_powers = [GAMMA_RATE ** (1 << bit) for bit in range(8)]
    for i in range(n_batch):
        facts = stats[i]
        into_r, into_a, opened, lengths, limit = [
            jnp.broadcast_to(facts[:, n : n + 1], (TILE, LANES)) for n in (0, 1, 4, 5, 6)
        ]
        powers = squarings(second_rate(lengths), 7)
        scale = powers[7] / lane_powers(powers[:7], lane)
        held[0, i] = into_r
        held[1, i] = into_a * scale
        held[2, i] = powers[7]
        held[3, i] = float(span - 1) - opened
        held[4, i] = limit

    def stores(j):
        cols = pl.ds(pl.multiple_of(j * LANES, LANES), LANES)
        return [
            pltpu.make_async_copy(source.at[j], target.at[:, cols], out_sem.at[1 + 2 * j + n])
            for n, (source, target) in enumerate(((done_r, gret_out), (done_a, gadv_out)))
        ]

    def column(step, scale_r):
        j = count - 1 - step
        cols = pl.ds(pl.multiple_of(j * LANES, LANES), LANES)
        place = lane_f + (j * LANES).astype(F32)
        for i in range(n_batch):
            carried = place > held[3, i]
            more = held[1, i]
            ret = bulk[i, :TILE, cols] + jnp.where(carried, scale_r, 0.0) * held[0, i]
            adv = bulk[i, TILE:, cols] + jnp.where(carried, more, 0.0)
            held[1, i] = more * held[2, i]
            rows = pl.ds(i, TILE, stride=n_batch)
            done_r[j, rows, :] = ret
            done_a[j, rows, :] = jnp.where(place < held[4, i], (adv - mean) * inverse, 0.0)
        for copy in stores(j):
            copy.start()
        return scale_r * gamma_powers[7]

    lax.fori_loop(0, count, column, gamma_powers[7] / lane_powers(gamma_powers[:7], lane))
    own_copy.wait()
    for j in range(count):
        for copy in stores(j):
            copy.wait()


def solution(mesh):
    n_tm, n_batch = mesh.shape["tm"], mesh.shape["batch"]

    def on_device(rewards, values, episode_ends, lengths, groups):
        height, span = rewards.shape
        block = pltpu.VMEM((height, span), F32)
        square = pltpu.VMEM((height, LANES), F32)
        turned = pltpu.VMEM((TILE * STRIDE, LANES), F32)
        out = jax.ShapeDtypeStruct((height, span), F32)

        def kernel(*refs):
            fused(n_tm, n_batch, *refs)

        own, bulk, stats = pl.pallas_call(
            kernel,
            out_shape=(
                pltpu.VMEM((height, span), F32),
                pltpu.VMEM((n_batch, 2 * TILE, span), F32),
                pltpu.VMEM((n_batch, TILE, LANES), F32),
            ),
            in_specs=[pl.BlockSpec(memory_space=pl.ANY)] * 5,
            out_specs=[pl.BlockSpec(memory_space=pltpu.VMEM)] * 3,
            scratch_shapes=[
                pltpu.VMEM((1, height), jnp.int32),
                pltpu.VMEM((1, height), jnp.int32),
                block,
                block,
                pltpu.VMEM((height, span), jnp.int32),
                turned,
                turned,
                pltpu.VMEM((TILE * STRIDE, LANES), jnp.int32),
                turned,
                turned,
                turned,
                pltpu.VMEM((n_batch, 2 * TILE, span), F32),
                pltpu.VMEM((TILE, LANES), F32),
                pltpu.VMEM((n_tm // 2, TILE, LANES), F32),
                square,
                pltpu.VMEM((TILE, LANES), F32),
                pltpu.VMEM((TILE, LANES), F32),
                pltpu.SemaphoreType.DMA((4, 3)),
                pltpu.SemaphoreType.DMA((2,)),
                pltpu.SemaphoreType.DMA,
                pltpu.SemaphoreType.DMA,
                pltpu.SemaphoreType.DMA,
                pltpu.SemaphoreType.DMA,
                pltpu.SemaphoreType.DMA,
                pltpu.SemaphoreType.DMA,
                pltpu.SemaphoreType.DMA,
                pltpu.SemaphoreType.DMA,
                pltpu.SemaphoreType.REGULAR,
            ],
            compiler_params=pltpu.CompilerParams(collective_id=0, has_side_effects=True),
        )(lengths.reshape(1, height), groups.reshape(1, height), rewards, values, episode_ends)
        columns = pltpu.VMEM((span // LANES, height, LANES), F32)
        return pl.pallas_call(
            finish,
            out_shape=(out, out, out),
            in_specs=[pl.BlockSpec(memory_space=pltpu.VMEM)] * 3,
            out_specs=[pl.BlockSpec(memory_space=pl.ANY)] * 3,
            scratch_shapes=[
                pltpu.VMEM((5, n_batch, TILE, LANES), F32),
                columns,
                columns,
                pltpu.SemaphoreType.DMA((1 + 2 * (span // LANES),)),
            ],
        )(*[pltpu.with_memory_space_constraint(a, pltpu.VMEM) for a in (own, bulk, stats)])

    return jax.shard_map(
        on_device,
        mesh=mesh,
        in_specs=(
            P("batch", "tm"),
            P("batch", "tm"),
            P("batch", "tm"),
            P("batch"),
            P("batch"),
        ),
        out_specs=(P("batch", "tm"), P("batch", "tm"), P("batch", "tm")),
        check_vma=False,
    )
```

```python
import math

import jax
import jax.numpy as jnp
from jax import lax
from jax.experimental import pallas as pl
from jax.experimental.pallas import tpu as pltpu
from jax.sharding import PartitionSpec as P

MESH = pl.DeviceIdType.MESH
F32 = jnp.float32
BF16 = jnp.bfloat16
GAMMA_RATE = 0.9995
ALPHA_RATE = 0.05
EPSILON = 1e-06
LANES = 128
TILE = 8
STRIDE = 136


def second_rate(lengths):
    return GAMMA_RATE * (1.0 - 1.0 / (ALPHA_RATE * lengths))


def squarings(rate, count):
    powers = [rate]
    for _ in range(count):
        powers.append(powers[-1] * powers[-1])
    return powers


def lane_powers(powers, exponent):
    result = None
    for bit, power in enumerate(powers):
        factor = jnp.where((exponent & (1 << bit)) != 0, power, 1.0)
        result = factor if result is None else result * factor
    return result


def joined(early, late):
    b_r, b_a, a_r, a_a, s_0, t_0, t_1, s_1, t_2 = early
    return [
        b_r + a_r * late[0],
        b_a + a_a * late[1],
        a_r * late[2],
        a_a * late[3],
        late[4] + s_0 + s_1 * late[1],
        late[5] + t_0 + late[1] * (2.0 * t_1 + t_2 * late[1]),
        late[6] + late[3] * (t_1 + t_2 * late[1]),
        late[7] + s_1 * late[3],
        late[8] + t_2 * late[3] * late[3],
    ]


def split(value, terms):
    pieces = []
    for _ in range(terms):
        piece = value.astype(BF16)
        pieces.append(piece)
        value = value - piece.astype(F32)
    return pieces


def fused(
    n_tm,
    n_batch,
    len_hbm,
    grp_hbm,
    rew_hbm,
    val_hbm,
    end_hbm,
    own_out,
    recv_bulk,
    recv_stat,
    len_ref,
    grp_ref,
    rew,
    val,
    end,
    time_rew,
    time_val,
    time_end,
    time_r,
    time_a,
    time_m,
    send_bulk,
    send_z,
    recv_z,
    send_stat,
    send_pair,
    recv_pair,
    in_sem,
    small_sem,
    pair_ss,
    pair_rs,
    bulk_ss,
    bulk_rs,
    z_ss,
    z_rs,
    stat_ss,
    stat_rs,
    ready_sem,
):
    height, span = rew.shape
    count = span // LANES
    chunks = 2
    chunk_cols = span // chunks
    tm = lax.axis_index("tm")
    me = lax.axis_index("batch")
    core = lax.rem(tm, 2)
    partner = tm + 1 - 2 * core
    start = tm * span
    chip = lax.div(tm, 2)
    n_chips = n_tm // 2
    side = math.isqrt(n_batch)
    row, column = lax.div(me, side), lax.rem(me, side)

    def away(distance, around):
        return min(distance, around - distance)

    steps = [(dx, dy) for dx in range(side) for dy in range(side) if dx or dy]
    steps.sort(key=lambda step: -away(step[0], side) - away(step[1], side))
    others = [lax.rem(row + dx, side) * side + lax.rem(column + dy, side) for dx, dy in steps]
    chip_steps = sorted(range(1, n_chips), key=lambda step: -away(step, n_chips))

    def loads(k):
        cols = pl.ds(k * chunk_cols, chunk_cols)
        return [
            pltpu.make_async_copy(source.at[:, cols], target.at[:, cols], in_sem.at[k, n])
            for n, (source, target) in enumerate(((rew_hbm, rew), (val_hbm, val), (end_hbm, end)))
        ]

    small = [
        pltpu.make_async_copy(source, target, small_sem.at[n])
        for n, (source, target) in enumerate(((len_hbm, len_ref), (grp_hbm, grp_ref)))
    ]
    for k in range(chunks):
        for copy in loads(k):
            copy.start()
    for copy in small:
        copy.start()

    barrier = pltpu.get_barrier_semaphore()
    for d in range(1, n_batch):
        pl.semaphore_signal(
            barrier,
            inc=1,
            device_id={"tm": tm - core, "batch": lax.rem(me + d, n_batch)},
            device_id_type=MESH,
        )
    for d in range(1, n_tm // 2):
        pl.semaphore_signal(
            barrier,
            inc=1,
            device_id={"tm": lax.rem(tm - core + 2 * d, n_tm) + 1, "batch": me},
            device_id_type=MESH,
        )
    pl.semaphore_signal(
        barrier, inc=1, device_id={"tm": partner, "batch": me}, device_id_type=MESH
    )

    for k in range(chunks):
        for copy in loads(k):
            copy.wait()
        for j in range(k * (count // chunks), (k + 1) * (count // chunks)):
            rows = pl.ds(j * STRIDE, LANES)
            for source, target in ((rew, time_rew), (val, time_val), (end, time_end)):
                target[rows, :] = source[:, j * LANES : (j + 1) * LANES].T

    for copy in small:
        copy.wait()
    lengths_row = len_ref[...]
    sublane = lax.broadcasted_iota(jnp.int32, (TILE, LANES), 0)
    lengths = jnp.broadcast_to(lengths_row, (TILE, LANES))
    limit = lengths - (start + sublane * LANES)
    rate = second_rate(lengths.astype(F32))
    whole_seg_a = squarings(rate, 7)[7]
    whole_seg_r = GAMMA_RATE**LANES

    def terms(k, value_next):
        at = pl.ds(k, TILE, stride=STRIDE)
        reward, value, ends = time_rew[at, :], time_val[at, :], time_end[at, :]
        inside = k < limit
        carry_on = (k < limit - 1) & (ends != 1)
        reward_in = jnp.where(inside, reward, 0.0)
        follow = jnp.where(carry_on, GAMMA_RATE * value_next, 0.0)
        delta = jnp.where(inside, reward_in + follow - value, 0.0)
        return at, value, carry_on, reward_in, delta

    def scan(step, carried):
        value_next, sum_r, sum_a, tail, totals = carried
        at, value, carry_on, reward_in, delta = terms(LANES - 1 - step, value_next)
        sum_r = reward_in + jnp.where(carry_on, GAMMA_RATE * sum_r, 0.0)
        sum_a = delta + jnp.where(carry_on, rate * sum_a, 0.0)
        tail = jnp.where(carry_on, rate * tail, 0.0)
        time_r[at, :] = sum_r
        time_a[at, :] = sum_a
        time_m[at, :] = tail
        more = (jnp.where(tail > 0.0, 1.0, 0.0), sum_a, sum_a * sum_a, sum_a * tail, tail, tail * tail)
        return value, sum_r, sum_a, tail, tuple(t + m for t, m in zip(totals, more))

    nought = limit.astype(F32) * 0.0
    first_value, head_r, head_a, _, totals = lax.fori_loop(
        0, LANES, scan, (nought, nought, nought, nought + 1.0, (nought,) * 6), unroll=8
    )
    head_a = head_a + first_value * (GAMMA_RATE / rate)
    seg_open = jnp.where(totals[0] == float(LANES), 1.0, 0.0)
    seg_r, seg_a = seg_open * whole_seg_r, seg_open * whole_seg_a
    tiles = (head_r, head_a, seg_r, seg_a) + totals[1:] + (totals[0], seg_open)
    done = None
    into_r = into_a = nought
    into_m = nought + 1.0
    for j in reversed(range(TILE)):
        segment = [jnp.broadcast_to(tile[j : j + 1], (TILE, LANES)) for tile in tiles]
        if done is None:
            done, opened, still_open = segment[:9], segment[9], segment[10]
            continue
        into_r = jnp.where(sublane == j, done[0], into_r)
        into_a = jnp.where(sublane == j, done[1], into_a)
        into_m = jnp.where(sublane == j, done[3], into_m)
        done = joined(segment[:9], done)
        opened = opened + still_open * segment[9]
        still_open = still_open * segment[10]
    send_z[...] = jnp.concatenate(
        [line[:1] for line in (done[0], done[1], opened, *done[4:])], axis=0
    )

    order = lax.broadcasted_iota(jnp.int32, (height, height), 0) == jnp.broadcast_to(
        grp_ref[...], (height, height)
    )
    order = jnp.where(order, 1.0, 0.0).astype(BF16)
    twice = jnp.concatenate([order, order], axis=1)
    thrice = jnp.concatenate([order, order, order], axis=1)
    wide = 2 * LANES

    def permute(c, _):
        cols = pl.ds(pl.multiple_of(c * wide, wide), wide)
        for n, source in enumerate((time_r, time_a)):
            parts = [
                source[pl.ds(pl.multiple_of((2 * c + h) * STRIDE, TILE), LANES), :] for h in (0, 1)
            ]
            pieces = jnp.concatenate(split(jnp.concatenate(parts, axis=0), 2), axis=1)
            moved = lax.dot_general(
                twice, pieces, (((1,), (1,)), ((), ())), preferred_element_type=F32
            )
            send_bulk[:, n * TILE : (n + 1) * TILE, cols] = moved.reshape(n_batch, TILE, wide)
        return 0


    @pl.when(core == 0)
    def _():
        pl.semaphore_wait(barrier, 2 * n_batch - 1)
        pl.semaphore_signal(
            ready_sem, inc=1, device_id={"tm": partner, "batch": me}, device_id_type=MESH
        )

    @pl.when(core == 1)
    def _():
        pl.semaphore_wait(ready_sem, 1)

    def bulk(to, slot):
        return pltpu.make_async_remote_copy(
            src_ref=send_bulk.at[to],
            dst_ref=recv_bulk.at[slot],
            send_sem=bulk_ss,
            recv_sem=bulk_rs,
            device_id={"tm": tm, "batch": to},
            device_id_type=MESH,
        )

    def send_all():
        left = LANES - lax.broadcasted_iota(jnp.int32, (LANES, LANES), 0)
        scale_r = lane_powers([GAMMA_RATE ** (1 << bit) for bit in range(8)], left)
        for j in range(TILE):
            rows = pl.ds(j * STRIDE, LANES)
            more_r, more_a, more_m = [
                jnp.broadcast_to(tile[j : j + 1], (LANES, LANES)) for tile in (into_r, into_a, into_m)
            ]
            tail = time_m[rows, :]
            time_r[rows, :] = time_r[rows, :] + jnp.where(tail > 0.0, scale_r, 0.0) * more_r
            time_a[rows, :] = time_a[rows, :] + tail * more_a
            time_m[rows, :] = tail * more_m
        lax.fori_loop(0, span // wide, permute, 0)
        for to in others:
            bulk(to, me).start()

    pair = pltpu.make_async_remote_copy(
        src_ref=send_z,
        dst_ref=recv_pair,
        send_sem=pair_ss,
        recv_sem=pair_rs,
        device_id={"tm": partner, "batch": me},
        device_id_type=MESH,
    )
    pair.start()


    @pl.when(tm < n_tm // 2)
    def _():
        send_all()

    @pl.when(core == 1)
    def _():
        pl.semaphore_wait(barrier, n_tm - 1)
        pl.semaphore_signal(
            ready_sem, inc=1, device_id={"tm": partner, "batch": me}, device_id_type=MESH
        )

    @pl.when(core == 0)
    def _():
        pl.semaphore_wait(ready_sem, 1)

    pair.wait()
    lengths_f = lengths_row.astype(F32)
    whole_a = jnp.broadcast_to(squarings(second_rate(lengths_f), 10)[10], (TILE, LANES))
    whole_r = GAMMA_RATE**span
    mine, theirs = send_z[...], recv_pair[...]

    def pieces_of(tile):
        return [jnp.broadcast_to(tile[n : n + 1], (TILE, LANES)) for n in range(TILE)]

    def block_of(tile):
        piece = pieces_of(tile)
        whole = jnp.where(piece[2] == float(span), 1.0, 0.0)
        return piece[:2] + [whole * whole_r, whole * whole_a] + piece[3:], whole

    early, early_open = block_of(jnp.where(core == 0, mine, theirs))
    late, late_open = block_of(jnp.where(core == 0, theirs, mine))
    both = joined(early, late)
    send_pair[...] = jnp.concatenate(
        [line[:1] for line in (both[0], both[1], early_open * late_open, *both[4:])], axis=0
    )
    recv_z[chip] = send_pair[...]

    def along(to, slot):
        return pltpu.make_async_remote_copy(
            src_ref=send_pair,
            dst_ref=recv_z.at[slot],
            send_sem=z_ss,
            recv_sem=z_rs,
            device_id={"tm": 2 * to + core, "batch": me},
            device_id_type=MESH,
        )

    for step in chip_steps:
        along(lax.rem(chip + step, n_chips), chip).start()

    @pl.when(tm >= n_tm // 2)
    def _():
        send_all()

    recv_bulk[me] = send_bulk[me]

    all_z = pltpu.make_async_remote_copy(
        src_ref=recv_z.at[pl.ds(0, n_chips - 1)],
        dst_ref=recv_z.at[pl.ds(0, n_chips - 1)],
        send_sem=z_ss,
        recv_sem=z_rs,
        device_id={"tm": partner, "batch": me},
        device_id_type=MESH,
    )
    all_z.wait_recv()

    both_r, both_a = whole_r * whole_r, whole_a * whole_a
    zero = whole_a * 0.0

    def chain(k, carried):
        block = n_chips - 1 - k
        into_r, into_a, own_r, own_a, first, second = carried
        piece = pieces_of(recv_z[block])
        here = jnp.where(block == chip, 1.0, 0.0)
        own_r = own_r + here * into_r
        own_a = own_a + here * into_a
        first = first + piece[3] + piece[6] * into_a
        second = second + piece[4] + into_a * (2.0 * piece[5] + piece[7] * into_a)
        into_r = piece[0] + piece[2] * both_r * into_r
        into_a = piece[1] + piece[2] * both_a * into_a
        return into_r, into_a, own_r, own_a, first, second

    _, _, own_r, own_a, first, second = lax.fori_loop(0, n_chips, chain, (zero,) * 6, unroll=4)
    is_early = jnp.where(core == 0, 1.0, 0.0)
    own_r = is_early * (late[0] + late[2] * own_r) + (1.0 - is_early) * own_r
    own_a = is_early * (late[1] + late[3] * own_a) + (1.0 - is_early) * own_a
    lines = jnp.concatenate(
        [line[:1] for line in (own_r, own_a, first, second, send_z[2:3], lengths_f)]
        + [lengths_f - start.astype(F32), jnp.zeros((height - 7, LANES), F32)],
        axis=0,
    )
    send_stat[...] = lax.dot_general(
        thrice,
        jnp.concatenate(split(lines, 3), axis=1),
        (((1,), (1,)), ((), ())),
        preferred_element_type=F32,
    )
    recv_stat[me] = send_stat[pl.ds(pl.multiple_of(me * TILE, TILE), TILE), :]

    def stat(to, slot):
        return pltpu.make_async_remote_copy(
            src_ref=send_stat.at[pl.ds(pl.multiple_of(to * TILE, TILE), TILE), :],
            dst_ref=recv_stat.at[slot],
            send_sem=stat_ss,
            recv_sem=stat_rs,
            device_id={"tm": tm, "batch": to},
            device_id_type=MESH,
        )

    for to in others:
        stat(to, me).start()

    own_into = jnp.broadcast_to(own_a[:1], (LANES, LANES))
    for j in range(count):
        rows = pl.ds(j * STRIDE, LANES)
        own_out[:, j * LANES : (j + 1) * LANES] = (time_a[rows, :] + time_m[rows, :] * own_into).T
    all_stats = pltpu.make_async_remote_copy(
        src_ref=recv_stat.at[pl.ds(0, n_batch - 1)],
        dst_ref=recv_stat.at[pl.ds(0, n_batch - 1)],
        send_sem=stat_ss,
        recv_sem=stat_rs,
        device_id={"tm": partner, "batch": me},
        device_id_type=MESH,
    )
    all_bulk = pltpu.make_async_remote_copy(
        src_ref=send_bulk.at[pl.ds(0, n_batch - 1)],
        dst_ref=recv_bulk.at[pl.ds(0, n_batch - 1)],
        send_sem=bulk_ss,
        recv_sem=bulk_rs,
        device_id={"tm": partner, "batch": me},
        device_id_type=MESH,
    )
    all_stats.wait()
    all_bulk.wait()
    all_z.wait_send()


def finish(own, bulk, stats, adv_out, gadv_out, gret_out, held, done_r, done_a, out_sem):
    n_batch = bulk.shape[0]
    span = bulk.shape[2]
    count = span // LANES
    own_copy = pltpu.make_async_copy(own, adv_out, out_sem.at[0])
    own_copy.start()
    total = stats[0]
    for i in range(1, n_batch):
        total = total + stats[i]
    counted = total[:, 5:6]
    mean = total[:, 2:3] / counted
    var = total[:, 3:4] / counted - mean * mean
    mean = jnp.broadcast_to(mean, (TILE, LANES))
    inverse = jnp.broadcast_to(1.0 / jnp.sqrt(var + EPSILON), (TILE, LANES))
    lane = lax.broadcasted_iota(jnp.int32, (TILE, LANES), 1)
    lane_f = lane.astype(F32)
    gamma_powers = [GAMMA_RATE ** (1 << bit) for bit in range(8)]
    for i in range(n_batch):
        facts = stats[i]
        into_r, into_a, opened, lengths, limit = [
            jnp.broadcast_to(facts[:, n : n + 1], (TILE, LANES)) for n in (0, 1, 4, 5, 6)
        ]
        powers = squarings(second_rate(lengths), 7)
        scale = powers[7] / lane_powers(powers[:7], lane)
        held[0, i] = into_r
        held[1, i] = into_a * scale
        held[2, i] = powers[7]
        held[3, i] = float(span - 1) - opened
        held[4, i] = limit

    def stores(j):
        cols = pl.ds(pl.multiple_of(j * LANES, LANES), LANES)
        return [
            pltpu.make_async_copy(source.at[j], target.at[:, cols], out_sem.at[1 + n])
            for n, (source, target) in enumerate(((done_r, gret_out), (done_a, gadv_out)))
        ]

    def column(step, scale_r):
        j = count - 1 - step
        cols = pl.ds(pl.multiple_of(j * LANES, LANES), LANES)
        place = lane_f + (j * LANES).astype(F32)
        for i in range(n_batch):
            carried = place > held[3, i]
            more = held[1, i]
            ret = bulk[i, :TILE, cols] + jnp.where(carried, scale_r, 0.0) * held[0, i]
            adv = bulk[i, TILE:, cols] + jnp.where(carried, more, 0.0)
            held[1, i] = more * held[2, i]
            rows = pl.ds(i, TILE, stride=n_batch)
            done_r[j, rows, :] = ret
            done_a[j, rows, :] = jnp.where(place < held[4, i], (adv - mean) * inverse, 0.0)
        for copy in stores(j):
            copy.start()
        return scale_r * gamma_powers[7]

    lax.fori_loop(0, count, column, gamma_powers[7] / lane_powers(gamma_powers[:7], lane))
    own_copy.wait()
    pltpu.make_async_copy(own, gret_out, out_sem.at[1]).wait()
    pltpu.make_async_copy(own, gadv_out, out_sem.at[2]).wait()


def solution(mesh):
    n_tm, n_batch = mesh.shape["tm"], mesh.shape["batch"]

    def on_device(rewards, values, episode_ends, lengths, groups):
        height, span = rewards.shape
        block = pltpu.VMEM((height, span), F32)
        square = pltpu.VMEM((height, LANES), F32)
        turned = pltpu.VMEM((TILE * STRIDE, LANES), F32)
        out = jax.ShapeDtypeStruct((height, span), F32)

        def kernel(*refs):
            fused(n_tm, n_batch, *refs)

        own, bulk, stats = pl.pallas_call(
            kernel,
            out_shape=(
                pltpu.VMEM((height, span), F32),
                pltpu.VMEM((n_batch, 2 * TILE, span), F32),
                pltpu.VMEM((n_batch, TILE, LANES), F32),
            ),
            in_specs=[pl.BlockSpec(memory_space=pl.ANY)] * 5,
            out_specs=[pl.BlockSpec(memory_space=pltpu.VMEM)] * 3,
            scratch_shapes=[
                pltpu.VMEM((1, height), jnp.int32),
                pltpu.VMEM((1, height), jnp.int32),
                block,
                block,
                pltpu.VMEM((height, span), jnp.int32),
                turned,
                turned,
                pltpu.VMEM((TILE * STRIDE, LANES), jnp.int32),
                turned,
                turned,
                turned,
                pltpu.VMEM((n_batch, 2 * TILE, span), F32),
                pltpu.VMEM((TILE, LANES), F32),
                pltpu.VMEM((n_tm // 2, TILE, LANES), F32),
                square,
                pltpu.VMEM((TILE, LANES), F32),
                pltpu.VMEM((TILE, LANES), F32),
                pltpu.SemaphoreType.DMA((2, 3)),
                pltpu.SemaphoreType.DMA((2,)),
                pltpu.SemaphoreType.DMA,
                pltpu.SemaphoreType.DMA,
                pltpu.SemaphoreType.DMA,
                pltpu.SemaphoreType.DMA,
                pltpu.SemaphoreType.DMA,
                pltpu.SemaphoreType.DMA,
                pltpu.SemaphoreType.DMA,
                pltpu.SemaphoreType.DMA,
                pltpu.SemaphoreType.REGULAR,
            ],
            compiler_params=pltpu.CompilerParams(collective_id=0, has_side_effects=True),
        )(lengths.reshape(1, height), groups.reshape(1, height), rewards, values, episode_ends)
        columns = pltpu.VMEM((span // LANES, height, LANES), F32)
        return pl.pallas_call(
            finish,
            out_shape=(out, out, out),
            in_specs=[pl.BlockSpec(memory_space=pltpu.VMEM)] * 3,
            out_specs=[pl.BlockSpec(memory_space=pl.ANY)] * 3,
            scratch_shapes=[
                pltpu.VMEM((5, n_batch, TILE, LANES), F32),
                columns,
                columns,
                pltpu.SemaphoreType.DMA((3,)),
            ],
        )(*[pltpu.with_memory_space_constraint(a, pltpu.VMEM) for a in (own, bulk, stats)])

    return jax.shard_map(
        on_device,
        mesh=mesh,
        in_specs=(
            P("batch", "tm"),
            P("batch", "tm"),
            P("batch", "tm"),
            P("batch"),
            P("batch"),
        ),
        out_specs=(P("batch", "tm"), P("batch", "tm"), P("batch", "tm")),
        check_vma=False,
    )
```
